32 devices in a mesh: layer: 4 (over y, core), row: 4 (over z), col: 2 (over x).
Axes of the slice: x: 2, y: 2, z: 4, core: 2. Of those that a mesh axis runs over, the one named last changes fastest.
Arguments:
- left: float32 [2048, 1024], P('row', ('layer', 'col')), may hold values from -6 to 6
- right: float32 [1024, 32768], P(('layer', 'row'), 'col'), may hold values from -0.1875 to 0.1875
Outputs:
- product: float32 [2048, 32768], P(('row', 'layer'), 'col')
The draws below stay inside these ranges and needn't reach their ends.
All inputs are finite; a program needn't handle non-finite values.
Results may differ from the reference program's by a relative error of at most 0.000076.
Values sent between devices are 32-bit elements; how exact they have to be, the bound alone decides.
A program may use at most 128 MiB of HBM per device.

```python
import jax
import jax.numpy as jnp
from jax import lax

NCOLS = 32768
K = 1024
M = 2048


def block_scale(key, dims, cuts, low, top_value):
    loudness = 1.0
    for position, parts in cuts:
        steps = jax.random.uniform(jax.random.fold_in(jax.random.fold_in(key, 6), position), (parts,), jnp.float32, low / len(cuts), top_value / len(cuts))
        loudness = loudness * jnp.repeat(jnp.exp(steps), dims[position] // parts).reshape((-1,) + (1,) * (len(dims) - 1 - position))
    return loudness


def bell_draw(stream_key, dims, width, limit, split=(), dtype=jnp.bfloat16):
    array = width * jax.random.normal(stream_key, dims, jnp.float32)
    if split:
        array = array * block_scale(stream_key, dims, split, -0.22, 0.18)
    return jnp.clip(array, -limit, limit).astype(dtype)


def setup_inputs(seed: int = 0) -> dict:
    key_list = jax.random.split(jax.random.key(seed), 3)
    return {
        "left": bell_draw(key_list[0], (M, K), 1.0, 6.0, ((0, 4), (1, 8)), jnp.float32),
        "right": bell_draw(key_list[1], (K, NCOLS), K ** -0.5, 0.1875, ((0, 16), (1, 2)), jnp.float32),
    }


def reference(left, right):
    return jnp.dot(left, right, precision=lax.Precision.HIGHEST, preferred_element_type=jnp.float32)
```

```python
import functools

import jax
import jax.numpy as jnp
from jax import lax
from jax.experimental import pallas as pl
from jax.experimental.pallas import tpu as pltpu
from jax.sharding import PartitionSpec as P

MESH = pl.DeviceIdType.MESH
CORES = 2
TILES = 4
AHEAD = 2
LEAD = 2
RELAY = 1
OWN_FROM = 4
OUTER_AHEAD = 4


def kernel(sizes, left, right, out, a_f32, a_hi, a_lo, b_all, b_hi, b_lo, c_buf,
           a0_s, a1_s, a1_r, a2_s, a2_r, a3_s, a3_r, b1_s, b1_r, b2_s, b2_r, far_s, fwd_s, d_s, d_r):
    layers, rows, cols, chunks, width, tiles, big = sizes
    half = rows // 2
    chips = layers // CORES
    height, wide = left.shape
    fine = height // tiles
    block = height // layers
    l, z = lax.axis_index("layer"), lax.axis_index("row")
    x = lax.axis_index("col") if cols > 1 else 0
    y, c = l // CORES, l % CORES
    side = z // half
    base = side * half
    centre = half - 1 + side
    other = half - side
    own = z - base
    piece = l * cols + x
    is_centre = z == centre
    is_outer = jnp.logical_not(is_centre)
    sibling = y * CORES + (1 - c)
    own_from = min(OWN_FROM, chunks // 2)
    own_fetch = max(0, own_from - 1)

    def remote(src, dst, send, recv, **to):
        return pltpu.make_async_remote_copy(
            src_ref=src, dst_ref=dst, send_sem=send, recv_sem=recv, device_id=to, device_id_type=MESH)

    barrier = pltpu.get_barrier_semaphore()
    greeted = 0
    for i in range(half):
        row = base + lax.rem(own + i, half)
        for k in range(layers):
            if (i, k) != (0, 0):
                to = {"layer": lax.rem(l + k, layers), "row": row}
                pl.semaphore_signal(barrier, inc=1, device_id=to, device_id_type=MESH)
                greeted += 1
    for k in range(1, cols):
        for m in range(chips):
            to = {"layer": lax.rem(l + m * CORES, layers), "col": lax.rem(x + k, cols)}
            pl.semaphore_signal(barrier, inc=1, device_id=to, device_id_type=MESH)
            greeted += 1

    @pl.when(is_centre)
    def _():
        for i in range(half):
            pl.semaphore_signal(barrier, inc=1, device_id={"row": (1 - side) * half + i}, device_id_type=MESH)
        pl.semaphore_wait(barrier, greeted + half)

    @pl.when(is_outer)
    def _():
        pl.semaphore_signal(barrier, inc=1, device_id={"row": other}, device_id_type=MESH)
        pl.semaphore_wait(barrier, greeted + 1)

    def b1(j, k):
        q = lax.rem(l + k, layers)
        src = right.at[:, pl.ds(pl.multiple_of((q * chunks + j) * width, width), width)]
        if k == 0:
            return pltpu.make_async_copy(src, b_all.at[j, l, z], b1_r.at[j, 0])
        return remote(src, b_all.at[j, l, z], b1_s.at[j, k], b1_r.at[j, k], layer=q)

    def b1_start(j):
        for k in range(layers):
            b1(j, k).start()

    def b1_wait(j):
        b1(j, 0).wait()
        for k in range(1, layers):
            b1(j, k).wait_recv()

    def b2(j, s, send, to):
        return remote(b_all.at[j, :, s], b_all.at[j, :, s], send, b2_r.at[j, s], row=to)

    def b2_own(j):
        return b2(j, z, b2_s.at[j], jnp.where(is_centre, other, centre))

    def b2_far():
        return b2(0, z, far_s, other)

    def relay(j, i):
        s = base + lax.rem(own + i, half)
        return b2(j, s, fwd_s.at[j, i], other)

    def relay_step(j):
        for i in range(1, half):
            relay(j, i).wait_recv()
            relay(j, i).start()

    def b2_wait(j):
        for i in range(half):
            b2(j, (1 - side) * half + i, b2_s.at[j], other).wait_recv()

    def rows_of(t):
        if isinstance(t, int) and t == tiles:
            return pl.ds(0, height)
        return pl.ds(t * fine, fine)

    def a1(s, t):
        return remote(left.at[rows_of(t)], a_f32.at[s, piece, rows_of(t)], a1_s.at[t], a1_r.at[s, t], row=centre)

    def a2(s, t, m, k):
        to = {"layer": lax.rem(l + m * CORES, layers)}
        if cols > 1:
            to["col"] = lax.rem(x + k, cols)
        dst = a_f32.at[s, piece, rows_of(t)]
        src = left if t == tiles else dst
        return remote(src, dst, a2_s.at[s, t, m, k], a2_r.at[s, t, m, k], **to)

    peers = [(m, k) for m in range(chips) for k in range(cols) if (m, k) != (0, 0)]
    everyone = [(0, 0)] + peers

    def a3(s, t, m, k, core):
        ls = lax.rem(y + chips - m, chips) * CORES + core
        xs = lax.rem(x + cols - k, cols)
        at = a_f32.at[s, ls * cols + xs, rows_of(t)]
        src = left if t == tiles and (m, k) == (0, 0) else at
        return remote(src, at, a3_s.at[s, t, m, k], a3_r.at[s, t, m, k], layer=sibling)

    def local_a():
        return pltpu.make_async_copy(left, a_f32.at[own, piece], a0_s)

    def split_a(s, at):
        for p in range(layers * cols):
            a = a_f32[s, p, at]
            hi = a.astype(jnp.bfloat16)
            a_hi[s, at, p * wide:(p + 1) * wide] = hi
            a_lo[s, at, p * wide:(p + 1) * wide] = (a - hi.astype(jnp.float32)).astype(jnp.bfloat16)

    def split_b(j):
        b = b_all[j].reshape(b_hi.shape)
        hi = b.astype(jnp.bfloat16)
        b_hi[...] = hi
        b_lo[...] = (b - hi.astype(jnp.float32)).astype(jnp.bfloat16)

    def product(j, s, at):
        dot = functools.partial(jnp.dot, preferred_element_type=jnp.float32)
        ah, al = a_hi[s, at, :], a_lo[s, at, :]
        c_buf[j, s, at, :] = dot(al, b_hi[...]) + dot(ah, b_lo[...]) + dot(ah, b_hi[...])

    def columns(j, source):
        return pl.ds(pl.multiple_of((source * chunks + j) * width, width), width)

    def block_of(q):
        return pl.ds(pl.multiple_of(q * block, block), block)

    def send_out(j, s, q):
        return remote(c_buf.at[j, s, block_of(q)], out.at[:, columns(j, l)],
                      d_s.at[s, j, q], d_r.at[j, l], layer=q, row=base + s)

    def send_own(j, k):
        return send_out(j, own, lax.rem(l + k, layers))

    def came(j, source):
        return remote(c_buf.at[j, 0, block_of(0)], out.at[:, columns(j, source)],
                      d_s.at[0, j, 0], d_r.at[j, source], layer=l, row=centre)

    def product_other(j):
        for i in range(1, half):
            s = lax.rem(own + i, half)

            @pl.loop(0, height // big)
            def _(t):
                product(j, s, pl.ds(pl.multiple_of(t * big, big), big))
                for r in range(big // block):
                    send_out(j, s, t * (big // block) + r).start()

    def product_own(j):
        split_b(j)

        @pl.loop(0, height // big)
        def _(t):
            product(j, own, pl.ds(pl.multiple_of(t * big, big), big))
        for k in range(1, layers):
            send_own(j, k).start()
        out[:, columns(j, l)] = c_buf[j, own, block_of(l), :]

    def fetch_own():
        for m, k in peers:
            a2(own, tiles, m, k).wait_recv()
            a3(own, tiles, m, k, c).start()

    def finish_own():
        local_a().wait()
        for m, k in everyone:
            a3(own, tiles, m, k, 1 - c).wait_recv()

        @pl.loop(0, tiles)
        def _(t):
            split_a(own, pl.ds(pl.multiple_of(t * fine, fine), fine))

    def owns(j):
        def upto(n):
            return jnp.maximum(jnp.minimum(2 * (n - own_from), n), 0)

        @pl.loop(upto(j), upto(j + 1))
        def _(i):
            product_own(i)

    @pl.when(is_outer)
    def _():
        b1_start(0)
        for t in range(min(2, tiles)):
            a1(own, t).start()
        for j in range(1, min(OUTER_AHEAD, chunks)):
            b1_start(j)
        b1_wait(0)
        b2_far().start()
        for t in range(2, tiles):
            a1(own, t).start()
            if t == 2:
                b2_own(0).start()
        if tiles <= 2:
            b2_own(0).start()

        @pl.loop(1, chunks)
        def _(j):
            @pl.when(j + OUTER_AHEAD - 1 < chunks)
            def _():
                b1_start(j + OUTER_AHEAD - 1)
            b1_wait(j)
            b2_own(j).start()

    lead = min(LEAD, chunks - 1)
    relayed = min(RELAY, chunks - 1)
    begun = min(lead + AHEAD, chunks - 1)

    @pl.when(is_centre)
    def _():
        b1_start(0)
        local_a().start()
        if chunks > 1:
            b1_start(1)
        b1_wait(0)
        b2_own(0).start()
        for t in range(tiles):
            for i in range(1, half):
                s = lax.rem(own + i, half)
                a1(s, t).wait_recv()
                for m, k in peers:
                    a2(s, t, m, k).start()
                a3(s, t, 0, 0, c).start()
            if t == 0:
                for j in range(2, begun + 1):
                    b1_start(j)
            if t == 1:
                for j in range(1, lead + 1):
                    b1_wait(j)
                    b2_own(j).start()
        for m, k in peers:
            a2(own, tiles, m, k).start()
        a3(own, tiles, 0, 0, c).start()

        for t in range(tiles):
            for i in range(1, half):
                s = lax.rem(own + i, half)
                for m, k in peers:
                    a2(s, t, m, k).wait_recv()
                    a3(s, t, m, k, c).start()
                for m, k in everyone:
                    a3(s, t, m, k, 1 - c).wait_recv()
                split_a(s, rows_of(t))
            if t == 0:
                for i in range(1, half):
                    b2(0, base + lax.rem(own + i, half), b2_s.at[0], other).wait_recv()
                b2_wait(0)
                split_b(0)
            for i in range(1, half):
                s = lax.rem(own + i, half)
                product(0, s, rows_of(t))
                for r in range(fine // block):
                    send_out(0, s, t * (fine // block) + r).start()
        for j in range(1, relayed + 1):
            relay_step(j)
        if own_from == 0:
            fetch_own()
            finish_own()
            product_own(0)

        @pl.loop(1, chunks)
        def _(j):
            @pl.when(j + lead + AHEAD < chunks)
            def _():
                b1_start(j + lead + AHEAD)

            @pl.when(j + lead < chunks)
            def _():
                b1_wait(j + lead)
                b2_own(j + lead).start()

            @pl.when(j + relayed < chunks)
            def _():
                relay_step(j + relayed)

            @pl.when(j == max(own_fetch, 1))
            def _():
                fetch_own()
            b2_wait(j)
            split_b(j)
            product_other(j)

            @pl.when(j == own_from)
            def _():
                finish_own()
            owns(j)

    @pl.loop(0, chunks)
    def _(j):
        for k in range(1, layers):
            b1(j, k).wait_send()
            came(j, lax.rem(l + k, layers)).wait_recv()
        b2_own(j).wait_send()

        @pl.when(is_outer)
        def _():
            came(j, l).wait_recv()

        @pl.when(is_centre)
        def _():
            for k in range(1, layers):
                send_own(j, k).wait_send()
            for i in range(1, half):
                s = lax.rem(own + i, half)
                for q in range(layers):
                    send_out(j, s, q).wait_send()

                @pl.when(j > 0)
                def _():
                    relay(j, i).wait_send()

    @pl.when(is_outer)
    def _():
        b2_far().wait_send()
        for t in range(tiles):
            a1(own, t).wait_send()

    @pl.when(is_centre)
    def _():
        for m, k in peers:
            a2(own, tiles, m, k).wait_send()
        for m, k in everyone:
            a3(own, tiles, m, k, c).wait_send()
        for i in range(1, half):
            s = lax.rem(own + i, half)
            for t in range(tiles):
                for m, k in peers:
                    a2(s, t, m, k).wait_send()
                for m, k in everyone:
                    a3(s, t, m, k, c).wait_send()


def body(mesh, left, right):
    layers, rows, cols = mesh.shape["layer"], mesh.shape["row"], mesh.shape["col"]
    if left.shape[1] % 128:
        left = lax.all_gather(left, "col", axis=1, tiled=True)
        cols = 1
    height, wide = left.shape
    depth, across = right.shape
    share = across // layers
    width = max(128, share // 32)
    chunks = share // width
    half = rows // 2
    inner = depth * layers * rows
    dma = pltpu.SemaphoreType.DMA
    tiles = min(TILES, layers)
    sizes = (layers, rows, cols, chunks, width, tiles, min(256, height))
    chips = layers // CORES
    f32, bf16 = jnp.float32, jnp.bfloat16
    return pl.pallas_call(
        functools.partial(kernel, sizes),
        out_shape=pltpu.VMEM((height // layers, across), f32),
        in_specs=[pl.BlockSpec(memory_space=pltpu.HBM)] * 2,
        out_specs=pl.BlockSpec(memory_space=pltpu.VMEM),
        scratch_shapes=[
            pltpu.VMEM((half, layers * cols, height, wide), f32),
            pltpu.VMEM((half, height, inner), bf16),
            pltpu.VMEM((half, height, inner), bf16),
            pltpu.VMEM((chunks, layers, rows, depth, width), f32),
            pltpu.VMEM((inner, width), bf16),
            pltpu.VMEM((inner, width), bf16),
            pltpu.VMEM((chunks, half, height, width), f32),
            dma, dma((tiles,)), dma((half, tiles)),
            dma((half, tiles + 1, chips, cols)), dma((half, tiles + 1, chips, cols)),
            dma((half, tiles + 1, chips, cols)), dma((half, tiles + 1, chips, cols)),
            dma((chunks, layers)), dma((chunks, layers)),
            dma((chunks,)), dma((chunks, rows)), dma, dma((chunks, half)),
            dma((half, chunks, layers)), dma((chunks, layers)),
        ],
        compiler_params=pltpu.CompilerParams(
            collective_id=1, has_side_effects=True, vmem_limit_bytes=52 * 2**20),
    )(left, right)


def solution(mesh):
    in_specs = (P("row", ("layer", "col")), P(("layer", "row"), "col"))
    out_specs = P(("row", "layer"), "col")
    return jax.shard_map(
        functools.partial(body, mesh), mesh=mesh, in_specs=in_specs, out_specs=out_specs, check_vma=False)
```

```python
import functools

import jax
import jax.numpy as jnp
from jax import lax
from jax.experimental import pallas as pl
from jax.experimental.pallas import tpu as pltpu
from jax.sharding import PartitionSpec as P

MESH = pl.DeviceIdType.MESH
CORES = 2
TILES = 4
AHEAD = 2
LEAD = 2
RELAY = 1
OWN_FROM = 6
GROUP = 2
PACE = 8


def kernel(sizes, left, right, out, a_f32, a_hi, a_lo, b_all, b_hi, b_lo, c_buf,
           a0_s, a1_s, a1_r, a2_s, a2_r, a3_s, a3_r, b1_s, b1_r, b2_s, b2_r, d_s, d_r):
    layers, rows, cols, chunks, width, tiles, big, group = sizes
    half = rows // 2
    chips = layers // CORES
    height, wide = left.shape
    fine = height // tiles
    block = height // layers
    l, z = lax.axis_index("layer"), lax.axis_index("row")
    x = lax.axis_index("col") if cols > 1 else 0
    y, c = l // CORES, l % CORES
    side = z // half
    base = side * half
    centre = half - 1 + side
    other = half - side
    own = z - base
    piece = l * cols + x
    is_centre = z == centre
    is_outer = jnp.logical_not(is_centre)
    sibling = y * CORES + (1 - c)
    own_from = min(OWN_FROM, chunks // 2)
    own_fetch = max(0, own_from - 1)
    own_span = max(chunks - own_from - 1, 1)
    share = chunks * width
    lead = min(LEAD, chunks - 1)
    relayed = min(RELAY, chunks - 1)
    begun = min(lead + AHEAD, chunks - 1)
    ready = max(min(PACE, chunks) - 2, min(relayed + group, chunks))
    pace = max(min(PACE, chunks), ready)

    def remote(src, dst, send, recv, **to):
        return pltpu.make_async_remote_copy(
            src_ref=src, dst_ref=dst, send_sem=send, recv_sem=recv, device_id=to, device_id_type=MESH)

    barrier = pltpu.get_barrier_semaphore()
    greeted = 0
    for i in range(half):
        row = base + lax.rem(own + i, half)
        for k in range(layers):
            if (i, k) != (0, 0):
                to = {"layer": lax.rem(l + k, layers), "row": row}
                pl.semaphore_signal(barrier, inc=1, device_id=to, device_id_type=MESH)
                greeted += 1
    for k in range(1, cols):
        for m in range(chips):
            to = {"layer": lax.rem(l + m * CORES, layers), "col": lax.rem(x + k, cols)}
            pl.semaphore_signal(barrier, inc=1, device_id=to, device_id_type=MESH)
            greeted += 1

    @pl.when(is_centre)
    def _():
        for i in range(half):
            pl.semaphore_signal(barrier, inc=1, device_id={"row": (1 - side) * half + i}, device_id_type=MESH)
        pl.semaphore_wait(barrier, greeted + half)

    @pl.when(is_outer)
    def _():
        pl.semaphore_signal(barrier, inc=1, device_id={"row": other}, device_id_type=MESH)
        pl.semaphore_wait(barrier, greeted + 1)

    def b1(j, k):
        q = lax.rem(l + k, layers)
        src = right.at[:, pl.ds(pl.multiple_of((q * chunks + j) * width, width), width)]
        if k == 0:
            return pltpu.make_async_copy(src, b_all.at[j, l, z], b1_r.at[j])
        return remote(src, b_all.at[j, l, z], b1_s, b1_r.at[j], layer=q)

    def b1_start(j):
        for k in range(layers):
            b1(j, k).start()

    def b1_wait(j):
        whole = b_all.at[j, :, z]
        remote(whole, whole, b1_s, b1_r.at[j], layer=sibling).wait_recv()

    def b1_sent():
        most = right.at[:, pl.ds(0, (layers - 1) * share)]
        remote(most, most, b1_s, b1_r.at[0], layer=sibling).wait_send()

    def b2_own(j):
        at = b_all.at[j, :, z]
        to = jnp.where(is_centre, other, centre)
        return remote(at, at, b2_s.at[0], b2_r.at[j, is_centre.astype(jnp.int32)], row=to)

    def relay_step(j):
        near = b_all.at[j, :, pl.ds(0, half - 1)]
        remote(near, near, b2_s.at[1], b2_r.at[j, 0], row=other).wait_recv()
        for i in range(1, half):
            at = b_all.at[j, :, base + lax.rem(own + i, half)]
            remote(at, at, b2_s.at[1], b2_r.at[j, 1], row=other).start()

    def b2_wait(j):
        distant = b_all.at[j, :, pl.ds(0, half)]
        remote(distant, distant, b2_s.at[0], b2_r.at[j, 1], row=other).wait_recv()

    def b2_sent():
        at = b_all.at[:, :, 0]
        remote(at, at, b2_s.at[0], b2_r.at[0, 0], row=other).wait_send()

    def relays_sent():
        at = b_all.at[:, :, pl.ds(0, half - 1)]
        remote(at, at, b2_s.at[1], b2_r.at[0, 0], row=other).wait_send()

    def rows_of(t):
        if isinstance(t, int) and t == tiles:
            return pl.ds(0, height)
        return pl.ds(t * fine, fine)

    def a1(t):
        at = a_f32.at[own, piece, rows_of(t)]
        return remote(left.at[rows_of(t)], at, a1_s, a1_r.at[own, t], row=centre)

    def a1_came(i, t):
        at = a_f32.at[0, 0, rows_of(t)]
        remote(at, at, a1_s, a1_r.at[lax.rem(own + i, half), t], row=centre).wait_recv()

    peers = [(m, k) for m in range(chips) for k in range(cols) if (m, k) != (0, 0)]
    everyone = [(0, 0)] + peers

    def a2(i, t, m, k):
        to = {"layer": lax.rem(l + m * CORES, layers)}
        if cols > 1:
            to["col"] = lax.rem(x + k, cols)
        at = a_f32.at[lax.rem(own + i, half), piece, rows_of(t)]
        src = left.at[rows_of(t)] if i == 0 else at
        recv = a2_r.at[i, 0 if i == 0 else t, m, k]
        return remote(src, at, a2_s, recv, **to)

    def a2_came(i, t, m, k):
        at = a_f32.at[0, 0, rows_of(t)]
        remote(at, at, a2_s, a2_r.at[i, 0 if i == 0 else t, m, k], layer=sibling).wait_recv()

    def a3(i, t, m, k):
        ls = lax.rem(y + chips - m, chips) * CORES + c
        xs = lax.rem(x + cols - k, cols)
        at = a_f32.at[lax.rem(own + i, half), ls * cols + xs, rows_of(t)]
        src = left if i == 0 and (m, k) == (0, 0) else at
        return remote(src, at, a3_s, a3_r.at[i, 0 if i == 0 else t], layer=sibling)

    def a3_came(i, t):
        at = a_f32.at[0, pl.ds(0, chips * cols), rows_of(t)]
        remote(at, at, a3_s, a3_r.at[i, 0 if i == 0 else t], layer=sibling).wait_recv()

    def a_sent():
        gathered = a_f32.at[:, pl.ds(0, len(peers))]
        remote(gathered, gathered, a2_s, a3_r.at[0, 0], layer=sibling).wait_send()
        passed = a_f32.at[:, pl.ds(0, len(everyone))]
        remote(passed, passed, a3_s, a3_r.at[0, 0], layer=sibling).wait_send()

    def local_a():
        return pltpu.make_async_copy(left, a_f32.at[own, piece], a0_s)

    def split_a(s, at):
        for p in range(layers * cols):
            a = a_f32[s, p, at]
            hi = a.astype(jnp.bfloat16)
            a_hi[s, at, p * wide:(p + 1) * wide] = hi
            a_lo[s, at, p * wide:(p + 1) * wide] = (a - hi.astype(jnp.float32)).astype(jnp.bfloat16)

    def split_b(j):
        b = b_all[j].reshape(b_hi.shape)
        hi = b.astype(jnp.bfloat16)
        b_hi[...] = hi
        b_lo[...] = (b - hi.astype(jnp.float32)).astype(jnp.bfloat16)

    def product(j, s, at):
        dot = functools.partial(jnp.dot, preferred_element_type=jnp.float32)
        ah, al = a_hi[s, at, :], a_lo[s, at, :]
        c_buf[j, s, at, :] = dot(al, b_hi[...]) + dot(ah, b_lo[...]) + dot(ah, b_hi[...])

    def columns(j, source):
        return pl.ds(pl.multiple_of((source * chunks + j) * width, width), width)

    def block_of(q):
        return pl.ds(pl.multiple_of(q * block, block), block)

    def send_out(j, s, q, mine):
        slot = jnp.where(q == l, j // group, chunks // group)
        return remote(c_buf.at[j, s, block_of(q)], out.at[:, columns(j, l)],
                      d_s.at[mine], d_r.at[slot], layer=q, row=base + s)

    def came_group(g):
        part = out.at[:, pl.ds(0, group * width)]
        remote(part, part, d_s.at[0], d_r.at[g], layer=sibling).wait_recv()

    def came_rest():
        part = out.at[:, pl.ds(0, (layers - 1) * share)]
        remote(part, part, d_s.at[0], d_r.at[chunks // group], layer=sibling).wait_recv()

    def outs_sent():
        theirs = c_buf.at[:, pl.ds(0, half - 1)]
        remote(theirs, theirs, d_s.at[0], d_r.at[0], layer=sibling).wait_send()
        mine = c_buf.at[:, 0, pl.ds(0, (layers - 1) * block)]
        remote(mine, mine, d_s.at[1], d_r.at[0], layer=sibling).wait_send()

    def product_other(j):
        for i in range(1, half):
            s = lax.rem(own + i, half)

            @pl.loop(0, height // big)
            def _(i):
                t = lax.rem(i + y + c, height // big)
                product(j, s, pl.ds(pl.multiple_of(t * big, big), big))
                for r in range(big // block):
                    send_out(j, s, t * (big // block) + r, 0).start()

    def product_own(j):
        split_b(j)

        @pl.loop(0, height // big)
        def _(t):
            product(j, own, pl.ds(pl.multiple_of(t * big, big), big))
        for k in range(1, layers):
            send_out(j, own, lax.rem(l + k, layers), 1).start()
        out[:, columns(j, l)] = c_buf[j, own, block_of(l), :]

    def fetch_own():
        for m, k in peers:
            a2_came(0, tiles, m, k)
            a3(0, tiles, m, k).start()

    def finish_own():
        local_a().wait()
        a3_came(0, tiles)

        @pl.loop(0, tiles)
        def _(t):
            split_a(own, pl.ds(pl.multiple_of(t * fine, fine), fine))

    def owns(j):
        def upto(n):
            return jnp.maximum(jnp.minimum((n - own_from) * chunks // own_span, n), 0)

        @pl.loop(upto(j), upto(j + 1))
        def _(i):
            product_own(i)

    def own_tile(t):
        for m, k in peers:
            a2(0, t, m, k).start()

    @pl.when(is_outer)
    def _():
        b1_start(0)
        for t in range(min(2, tiles)):
            a1(t).start()
        for j in range(1, pace):
            b1_start(j)
        for j in range(ready):
            b1_wait(j)
            b2_own(j).start()
            if j == 0:
                for t in range(2, tiles):
                    a1(t).start()

        @pl.loop(0, chunks // group)
        def _(g):
            came_group(g)
            for i in range(group):
                j = g * group + i

                @pl.when(j + pace < chunks)
                def _():
                    b1_start(j + pace)

                @pl.when(j + ready < chunks)
                def _():
                    b1_wait(j + ready)
                    b2_own(j + ready).start()

    @pl.when(is_centre)
    def _():
        b1_start(0)
        for j in range(1, min(2, begun + 1)):
            b1_start(j)
        local_a().start()
        a3(0, tiles, 0, 0).start()
        for t in range(tiles):
            for i in range(1, half):
                a1_came(i, t)
                for m, k in peers:
                    a2(i, t, m, k).start()
                a3(i, t, 0, 0).start()
            if t == 0:
                b1_wait(0)
                b2_own(0).start()
            if t == 1:
                if begun >= 2:
                    b1_start(2)
                relay_step(0)
                if lead >= 1:
                    b1_wait(1)
                    b2_own(1).start()
        for j in range(3, begun + 1):
            b1_start(j)

        for t in range(tiles):
            for i in range(1, half):
                for m, k in peers:
                    a2_came(i, t, m, k)
                    a3(i, t, m, k).start()
                a3_came(i, t)
                split_a(lax.rem(own + i, half), rows_of(t))
            if t == 0:
                b2_wait(0)
                split_b(0)
            for i in range(1, half):
                s = lax.rem(own + i, half)
                product(0, s, rows_of(t))
                for r in range(fine // block):
                    send_out(0, s, t * (fine // block) + r, 0).start()
            if t == 0:
                for j in range(1, relayed + 1):
                    relay_step(j)
                for j in range(2, lead + 1):
                    b1_wait(j)
                    b2_own(j).start()
        own_tile(0)
        if own_fetch < tiles:
            for t in range(1, tiles):
                own_tile(t)
        if own_from == 0:
            fetch_own()
            finish_own()
            product_own(0)

        @pl.loop(1, chunks)
        def _(j):
            @pl.when(j + lead + AHEAD < chunks)
            def _():
                b1_start(j + lead + AHEAD)

            @pl.when(j + lead < chunks)
            def _():
                b1_wait(j + lead)
                b2_own(j + lead).start()

            @pl.when(j + relayed < chunks)
            def _():
                relay_step(j + relayed)

            if own_fetch >= tiles:
                @pl.when(j < tiles)
                def _():
                    own_tile(j)

            @pl.when(j == max(own_fetch, 1))
            def _():
                fetch_own()
            b2_wait(j)
            split_b(j)
            product_other(j)

            @pl.when(j == own_from)
            def _():
                finish_own()
            owns(j)

    b1_sent()
    b2_sent()

    @pl.when(is_outer)
    def _():
        remote(left, left, a1_s, a1_r.at[0, 0], row=centre).wait_send()

    @pl.when(is_centre)
    def _():
        a_sent()
        relays_sent()
        outs_sent()
    came_rest()


def body(mesh, left, right):
    layers, rows, cols = mesh.shape["layer"], mesh.shape["row"], mesh.shape["col"]
    if left.shape[1] % 128:
        left = lax.all_gather(left, "col", axis=1, tiled=True)
        cols = 1
    height, wide = left.shape
    depth, across = right.shape
    share = across // layers
    width = max(128, share // 32)
    chunks = share // width
    half = rows // 2
    inner = depth * layers * rows
    dma = pltpu.SemaphoreType.DMA
    tiles = min(TILES, layers)
    group = GROUP if chunks % GROUP == 0 else 1
    sizes = (layers, rows, cols, chunks, width, tiles, min(256, height), group)
    chips = layers // CORES
    f32, bf16 = jnp.float32, jnp.bfloat16
    return pl.pallas_call(
        functools.partial(kernel, sizes),
        out_shape=pltpu.VMEM((height // layers, across), f32),
        in_specs=[pl.BlockSpec(memory_space=pltpu.HBM)] * 2,
        out_specs=pl.BlockSpec(memory_space=pltpu.VMEM),
        scratch_shapes=[
            pltpu.VMEM((half, layers * cols, height, wide), f32),
            pltpu.VMEM((half, height, inner), bf16),
            pltpu.VMEM((half, height, inner), bf16),
            pltpu.VMEM((chunks, layers, rows, depth, width), f32),
            pltpu.VMEM((inner, width), bf16),
            pltpu.VMEM((inner, width), bf16),
            pltpu.VMEM((chunks, half, height, width), f32),
            dma, dma, dma((half, tiles)),
            dma, dma((half, tiles, chips, cols)), dma, dma((half, tiles)),
            dma, dma((chunks,)), dma((2,)), dma((chunks, 2)),
            dma((2,)), dma((chunks // group + 1,)),
        ],
        compiler_params=pltpu.CompilerParams(
            collective_id=1, has_side_effects=True, vmem_limit_bytes=52 * 2**20),
    )(left, right)


def solution(mesh):
    in_specs = (P("row", ("layer", "col")), P(("layer", "row"), "col"))
    out_specs = P(("row", "layer"), "col")
    return jax.shard_map(
        functools.partial(body, mesh), mesh=mesh, in_specs=in_specs, out_specs=out_specs, check_vma=False)
```

```python
import functools

import jax
import jax.numpy as jnp
from jax import lax
from jax.experimental import pallas as pl
from jax.experimental.pallas import tpu as pltpu
from jax.sharding import PartitionSpec as P

MESH = pl.DeviceIdType.MESH
CORES = 2
TILES = 4
AHEAD = 4
LEAD = 2
RELAY = 1
OWN_FROM = 7
GROUP = 2
DIRECT = 4
PACE = 8


def kernel(sizes, left, right, out, a_f32, a_hi, a_lo, b_all, b_hi, b_lo, c_buf,
           a0_s, a1_s, a1_r, a2_s, a2_r, a3_s, a3_r, b1_s, b1_r, b2_s, b2_r, e_r, f_s, f_r, d_s, d_r):
    layers, rows, cols, chunks, width, tiles, big, group, fill = sizes
    half = rows // 2
    chips = layers // CORES
    height, wide = left.shape
    fine = height // tiles
    block = height // layers
    l, z = lax.axis_index("layer"), lax.axis_index("row")
    x = lax.axis_index("col") if cols > 1 else 0
    y, c = l // CORES, l % CORES
    side = z // half
    base = side * half
    centre = half - 1 + side
    other = half - side
    own = z - base
    piece = l * cols + x
    is_centre = z == centre
    is_outer = jnp.logical_not(is_centre)
    sibling = y * CORES + (1 - c)
    own_from = min(OWN_FROM, chunks // 2)
    own_fetch = max(0, own_from - 1)
    own_span = max(chunks - own_from - 1, 1)
    share = chunks * width
    lead = min(LEAD, chunks - 1)
    relayed = min(RELAY, chunks - 1)
    begun = min(lead + AHEAD, chunks - 1)
    direct = min(DIRECT, lead + fill + 1)
    ready = max(min(PACE, chunks) - 2, min(relayed + group, chunks))
    pace = max(min(PACE, chunks), ready)

    def remote(src, dst, send, recv, **to):
        return pltpu.make_async_remote_copy(
            src_ref=src, dst_ref=dst, send_sem=send, recv_sem=recv, device_id=to, device_id_type=MESH)

    barrier = pltpu.get_barrier_semaphore()
    greeted = 0
    for i in range(half):
        row = base + lax.rem(own + i, half)
        for k in range(layers):
            if (i, k) != (0, 0):
                to = {"layer": lax.rem(l + k, layers), "row": row}
                pl.semaphore_signal(barrier, inc=1, device_id=to, device_id_type=MESH)
                greeted += 1
    for k in range(1, cols):
        for m in range(chips):
            to = {"layer": lax.rem(l + m * CORES, layers), "col": lax.rem(x + k, cols)}
            pl.semaphore_signal(barrier, inc=1, device_id=to, device_id_type=MESH)
            greeted += 1

    @pl.when(is_centre)
    def _():
        for i in range(half):
            pl.semaphore_signal(barrier, inc=1, device_id={"row": (1 - side) * half + i}, device_id_type=MESH)
        pl.semaphore_wait(barrier, greeted + half)

    @pl.when(is_outer)
    def _():
        pl.semaphore_signal(barrier, inc=1, device_id={"row": other}, device_id_type=MESH)
        pl.semaphore_wait(barrier, greeted + 1)

    def b1(j, k):
        q = lax.rem(l + k, layers)
        src = right.at[:, pl.ds(pl.multiple_of((q * chunks + j) * width, width), width)]
        if k == 0:
            return pltpu.make_async_copy(src, b_all.at[j, l, z], b1_r.at[j])
        return remote(src, b_all.at[j, l, z], b1_s, b1_r.at[j], layer=q)

    def b1_start(j):
        for k in range(layers):
            b1(j, k).start()

    def b1_wait(j):
        whole = b_all.at[j, :, z]
        remote(whole, whole, b1_s, b1_r.at[j], layer=sibling).wait_recv()

    def b1_sent():
        most = right.at[:, pl.ds(0, (layers - 1) * share)]
        remote(most, most, b1_s, b1_r.at[0], layer=sibling).wait_send()

    def near(j):
        at = b_all.at[j, :, z]
        return remote(at, at, b2_s.at[0], b2_r.at[j, 0], row=centre)

    def far(j):
        at = b_all.at[j, :, z]
        return remote(at, at, b2_s.at[0], b2_r.at[j, 1], row=other)

    def far_part(j, k):
        q = lax.rem(l + k, layers)
        at = b_all.at[j, q, z]
        src = right.at[:, columns(j, l)] if k == 0 else at
        recv = e_r if fill and j == 0 else b2_r.at[j, 1]
        return remote(src, at, b2_s.at[0], recv, row=other)

    def far_rest(j):
        b1_wait(j)
        if j < direct:
            for k in range(1, layers):
                far_part(j, k).start()
        else:
            far(j).start()

    def fill_send(row):
        at = b_all.at[0, :, row]
        remote(at, at, f_s, f_r, row=base + (1 - own)).start()

    def fill_own():
        fill_send(z)

    def fill_far():
        at = b_all.at[0, :, 0]
        remote(at, at, b2_s.at[0], e_r, row=other).wait_recv()
        fill_send(other)

    def fill_relayed():
        at = b_all.at[0, :, pl.ds(0, half - 1)]
        remote(at, at, b2_s.at[0], b2_r.at[0, 1], row=other).wait_recv()
        fill_send((1 - side) * (rows - 1))

    def fill_came():
        at = b_all.at[0, :, pl.ds(0, rows - 1)]
        remote(at, at, f_s, f_r, row=centre).wait_recv()

    def fill_sent():
        at = b_all.at[0, :, pl.ds(0, rows - 1)]
        remote(at, at, f_s, f_r, row=centre).wait_send()

    def relay_step(j):
        near = b_all.at[j, :, pl.ds(0, half - 1)]
        remote(near, near, b2_s.at[1], b2_r.at[j, 0], row=other).wait_recv()
        for i in range(1, half):
            at = b_all.at[j, :, base + lax.rem(own + i, half)]
            remote(at, at, b2_s.at[1], b2_r.at[j, 1], row=other).start()

    def b2_wait(j):
        distant = b_all.at[j, :, pl.ds(0, half)]
        remote(distant, distant, b2_s.at[0], b2_r.at[j, 1], row=other).wait_recv()

    def b2_sent():
        at = b_all.at[:, :, 0]
        remote(at, at, b2_s.at[0], b2_r.at[0, 0], row=other).wait_send()

    def relays_sent():
        at = b_all.at[:, :, pl.ds(0, half - 1)]
        remote(at, at, b2_s.at[1], b2_r.at[0, 0], row=other).wait_send()

    def rows_of(t):
        if isinstance(t, int) and t == tiles:
            return pl.ds(0, height)
        return pl.ds(t * fine, fine)

    def a1(t):
        at = a_f32.at[own, piece, rows_of(t)]
        return remote(left.at[rows_of(t)], at, a1_s, a1_r.at[own, t], row=centre)

    def a1_came(i, t):
        at = a_f32.at[0, 0, rows_of(t)]
        remote(at, at, a1_s, a1_r.at[lax.rem(own + i, half), t], row=centre).wait_recv()

    peers = [(m, k) for m in range(chips) for k in range(cols) if (m, k) != (0, 0)]
    everyone = [(0, 0)] + peers

    def a2(i, t, m, k):
        to = {"layer": lax.rem(l + m * CORES, layers)}
        if cols > 1:
            to["col"] = lax.rem(x + k, cols)
        at = a_f32.at[lax.rem(own + i, half), piece, rows_of(t)]
        src = left.at[rows_of(t)] if i == 0 else at
        recv = a2_r.at[i, 0 if i == 0 else t, m, k]
        return remote(src, at, a2_s, recv, **to)

    def a2_came(i, t, m, k):
        at = a_f32.at[0, 0, rows_of(t)]
        remote(at, at, a2_s, a2_r.at[i, 0 if i == 0 else t, m, k], layer=sibling).wait_recv()

    def a3(i, t, m, k):
        ls = lax.rem(y + chips - m, chips) * CORES + c
        xs = lax.rem(x + cols - k, cols)
        at = a_f32.at[lax.rem(own + i, half), ls * cols + xs, rows_of(t)]
        src = left if i == 0 and (m, k) == (0, 0) else at
        return remote(src, at, a3_s, a3_r.at[i, 0 if i == 0 else t], layer=sibling)

    def a3_came(i, t):
        at = a_f32.at[0, pl.ds(0, chips * cols), rows_of(t)]
        remote(at, at, a3_s, a3_r.at[i, 0 if i == 0 else t], layer=sibling).wait_recv()

    def a_sent(count):
        gathered = a_f32.at[pl.ds(0, count), pl.ds(0, len(peers))]
        remote(gathered, gathered, a2_s, a3_r.at[0, 0], layer=sibling).wait_send()
        passed = a_f32.at[pl.ds(0, count), pl.ds(0, len(everyone))]
        remote(passed, passed, a3_s, a3_r.at[0, 0], layer=sibling).wait_send()

    def local_a():
        return pltpu.make_async_copy(left, a_f32.at[own, piece], a0_s)

    def split_a(s, at):
        for p in range(layers * cols):
            a = a_f32[s, p, at]
            hi = a.astype(jnp.bfloat16)
            a_hi[s, at, p * wide:(p + 1) * wide] = hi
            a_lo[s, at, p * wide:(p + 1) * wide] = (a - hi.astype(jnp.float32)).astype(jnp.bfloat16)

    def split_b(j):
        b = b_all[j].reshape(b_hi.shape)
        hi = b.astype(jnp.bfloat16)
        b_hi[...] = hi
        b_lo[...] = (b - hi.astype(jnp.float32)).astype(jnp.bfloat16)

    def product(j, s, at):
        dot = functools.partial(jnp.dot, preferred_element_type=jnp.float32)
        ah, al = a_hi[s, at, :], a_lo[s, at, :]
        c_buf[j, s, at, :] = dot(al, b_hi[...]) + dot(ah, b_lo[...]) + dot(ah, b_hi[...])

    def columns(j, source):
        return pl.ds(pl.multiple_of((source * chunks + j) * width, width), width)

    def block_of(q):
        return pl.ds(pl.multiple_of(q * block, block), block)

    def send_out(j, s, q, mine):
        slot = jnp.where(q == l, j // group, chunks // group)
        return remote(c_buf.at[j, s, block_of(q)], out.at[:, columns(j, l)],
                      d_s.at[mine], d_r.at[slot], layer=q, row=base + s)

    def came_group(g, count):
        part = out.at[:, pl.ds(0, count * width)]
        remote(part, part, d_s.at[0], d_r.at[g], layer=sibling).wait_recv()

    def came_rest():
        part = out.at[:, pl.ds(0, (layers - 1) * share)]
        remote(part, part, d_s.at[0], d_r.at[chunks // group], layer=sibling).wait_recv()

    def outs_sent():
        theirs = c_buf.at[pl.ds(0, chunks - fill), pl.ds(0, half - 1)]
        remote(theirs, theirs, d_s.at[0], d_r.at[0], layer=sibling).wait_send()
        mine = c_buf.at[:, 0, pl.ds(0, (layers - 1) * block)]
        remote(mine, mine, d_s.at[1], d_r.at[0], layer=sibling).wait_send()

    def product_other(j):
        for i in range(1, half):
            s = lax.rem(own + i, half)

            @pl.loop(0, height // big)
            def _(i):
                t = lax.rem(i + y + c, height // big)
                product(j, s, pl.ds(pl.multiple_of(t * big, big), big))
                for r in range(big // block):
                    send_out(j, s, t * (big // block) + r, 0).start()

    def product_own(j):
        split_b(j)

        @pl.loop(0, height // big)
        def _(t):
            product(j, own, pl.ds(pl.multiple_of(t * big, big), big))
        for k in range(1, layers):
            send_out(j, own, lax.rem(l + k, layers), 1).start()
        out[:, columns(j, l)] = c_buf[j, own, block_of(l), :]

    def fetch_own():
        for m, k in peers:
            a2_came(0, tiles, m, k)
            a3(0, tiles, m, k).start()

    def finish_own():
        local_a().wait()
        a3_came(0, tiles)

        @pl.loop(0, tiles)
        def _(t):
            split_a(own, pl.ds(pl.multiple_of(t * fine, fine), fine))

    def owns(j):
        def upto(n):
            return jnp.maximum(jnp.minimum((n - own_from) * chunks // own_span, n), 0)

        @pl.loop(upto(j), upto(j + 1))
        def _(i):
            product_own(i)

    def own_tile(t):
        for m, k in peers:
            a2(0, t, m, k).start()

    def outer_step(g):
        for i in range(group):
            j = g * group + i

            @pl.when(j + pace < chunks)
            def _():
                b1_start(j + pace)

            @pl.when(j + ready < chunks)
            def _():
                b1_wait(j + ready)
                near(j + ready).start()

    @pl.when(is_outer)
    def _():
        b1_start(0)
        for t in range(min(2, tiles)):
            a1(t).start()
        for j in range(1, min(3, pace)):
            b1_start(j)
        if fill:
            local_a().start()
            a3(0, tiles, 0, 0).start()
        for j in range(3, pace):
            if fill and j - 3 < tiles:
                own_tile(j - 3)
            b1_start(j)
        if fill:
            for t in range(max(pace - 3, 0), tiles):
                own_tile(t)
        for j in range(ready):
            b1_wait(j)
            near(j).start()
            if j == min(1, ready - 1):
                for t in range(2, tiles):
                    a1(t).start()
        if fill:
            fetch_own()
            finish_own()
            fill_came()
            product_own(0)
            came_group(0, group - fill)
            outer_step(0)

        @pl.loop(fill, chunks // group)
        def _(g):
            came_group(g, group)
            outer_step(g)

    @pl.when(is_centre)
    def _():
        b1_start(0)
        for j in range(direct):
            far_part(j, 0).start()
        for j in range(1, min(2, begun + 1)):
            b1_start(j)
        local_a().start()
        a3(0, tiles, 0, 0).start()
        def spread(t):
            for i in range(1, half):
                a1_came(i, t)
                for m, k in peers:
                    a2(i, t, m, k).start()
                a3(i, t, 0, 0).start()

        def pass_on(t):
            for i in range(1, half):
                for m, k in peers:
                    a2_came(i, t, m, k)
                    a3(i, t, m, k).start()

        spread(0)
        far_rest(0)
        if fill:
            fill_own()
        if tiles > 1:
            spread(1)
        if begun >= 2:
            b1_start(2)
        if lead >= 1:
            far_rest(1)
        relay_step(0)
        if fill:
            fill_far()
        pass_on(0)
        if fill:
            relay_step(1)
        for t in range(2, tiles):
            spread(t)
            if t == 2:
                pass_on(1)
        if tiles == 2:
            pass_on(1)
        for j in range(3, begun + 1):
            b1_start(j)

        for t in range(tiles):
            for i in range(1, half):
                a3_came(i, t)
                split_a(lax.rem(own + i, half), rows_of(t))
            if t == 0:
                if fill:
                    fill_relayed()
                b2_wait(fill)
                split_b(fill)
            for i in range(1, half):
                s = lax.rem(own + i, half)
                product(fill, s, rows_of(t))
                for r in range(fine // block):
                    send_out(fill, s, t * (fine // block) + r, 0).start()
            if t == 0:
                for j in range(2, lead + 1):
                    far_rest(j)
                for j in range(1 + fill, relayed + fill + 1):
                    relay_step(j)
            if 2 <= t + 2 < tiles:
                pass_on(t + 2)
            if t == min(2, tiles - 1):
                for j in range(lead + 1, lead + fill + 1):
                    far_rest(j)
        own_tile(0)
        if own_fetch < tiles:
            for t in range(1, tiles):
                own_tile(t)
        if own_from == 0:
            fetch_own()
            finish_own()
            product_own(0)

        @pl.loop(1 + fill, chunks)
        def _(j):
            @pl.when(j + lead + AHEAD - fill < chunks)
            def _():
                b1_start(j + lead + AHEAD - fill)

            @pl.when(j + relayed < chunks)
            def _():
                relay_step(j + relayed)

            @pl.when(j + lead < chunks)
            def _():
                b1_wait(j + lead)
                far(j + lead).start()

            if own_fetch >= tiles:
                @pl.when(j - fill < tiles)
                def _():
                    own_tile(j - fill)

            @pl.when(j == max(own_fetch, 1))
            def _():
                fetch_own()
            b2_wait(j)
            split_b(j)
            product_other(j)

            @pl.when(j == own_from)
            def _():
                finish_own()
            owns(j)

    b1_sent()
    b2_sent()

    @pl.when(is_outer)
    def _():
        remote(left, left, a1_s, a1_r.at[0, 0], row=centre).wait_send()
        if fill:
            a_sent(1)
            mine = c_buf.at[0, 0, pl.ds(0, (layers - 1) * block)]
            remote(mine, mine, d_s.at[1], d_r.at[0], layer=sibling).wait_send()

    @pl.when(is_centre)
    def _():
        a_sent(half)
        if fill:
            fill_sent()
        relays_sent()
        outs_sent()
    came_rest()


def body(mesh, left, right):
    layers, rows, cols = mesh.shape["layer"], mesh.shape["row"], mesh.shape["col"]
    if left.shape[1] % 128:
        left = lax.all_gather(left, "col", axis=1, tiled=True)
        cols = 1
    height, wide = left.shape
    depth, across = right.shape
    share = across // layers
    width = max(128, share // 32)
    chunks = share // width
    half = rows // 2
    inner = depth * layers * rows
    dma = pltpu.SemaphoreType.DMA
    tiles = min(TILES, layers)
    group = GROUP if chunks % GROUP == 0 else 1
    fill = 1 if half == 2 and group == 2 and chunks >= 2 * OWN_FROM else 0
    sizes = (layers, rows, cols, chunks, width, tiles, min(256, height), group, fill)
    chips = layers // CORES
    f32, bf16 = jnp.float32, jnp.bfloat16
    return pl.pallas_call(
        functools.partial(kernel, sizes),
        out_shape=pltpu.VMEM((height // layers, across), f32),
        in_specs=[pl.BlockSpec(memory_space=pltpu.HBM)] * 2,
        out_specs=pl.BlockSpec(memory_space=pltpu.VMEM),
        scratch_shapes=[
            pltpu.VMEM((half, layers * cols, height, wide), f32),
            pltpu.VMEM((half, height, inner), bf16),
            pltpu.VMEM((half, height, inner), bf16),
            pltpu.VMEM((chunks, layers, rows, depth, width), f32),
            pltpu.VMEM((inner, width), bf16),
            pltpu.VMEM((inner, width), bf16),
            pltpu.VMEM((chunks, half, height, width), f32),
            dma, dma, dma((half, tiles)),
            dma, dma((half, tiles, chips, cols)), dma, dma((half, tiles)),
            dma, dma((chunks,)), dma((2,)), dma((chunks, 2)),
            dma, dma, dma,
            dma((2,)), dma((chunks // group + 1,)),
        ],
        compiler_params=pltpu.CompilerParams(
            collective_id=1, has_side_effects=True, vmem_limit_bytes=52 * 2**20),
    )(left, right)


def solution(mesh):
    in_specs = (P("row", ("layer", "col")), P(("layer", "row"), "col"))
    out_specs = P(("row", "layer"), "col")
    return jax.shard_map(
        functools.partial(body, mesh), mesh=mesh, in_specs=in_specs, out_specs=out_specs, check_vma=False)
```

```python
import functools

import jax
import jax.numpy as jnp
from jax import lax
from jax.experimental import pallas as pl
from jax.experimental.pallas import tpu as pltpu
from jax.sharding import PartitionSpec as P

MESH = pl.DeviceIdType.MESH
CORES = 2
TILES = 4
AHEAD = 4
LEAD = 2
RELAY = 2
OWN_FROM = 7
GROUP = 2
DIRECT = 4
FILL = 2
PACE = 10


def kernel(sizes, left, right, out, a_f32, a_hi, a_lo, b_all, b_hi, b_lo, c_buf, early,
           e_s, a0_s, a1_s, a1_r, a2_s, a2_r, a3_s, a3_r, b1_s, b1_r, b2_s, b2_r, e_r, f_s, f_r, d_s, d_r):
    layers, rows, cols, chunks, width, tiles, big, group, fill = sizes
    half = rows // 2
    chips = layers // CORES
    height, wide = left.shape
    fine = height // tiles
    block = height // layers
    l, z = lax.axis_index("layer"), lax.axis_index("row")
    x = lax.axis_index("col") if cols > 1 else 0
    y, c = l // CORES, l % CORES
    side = z // half
    base = side * half
    centre = half - 1 + side
    other = half - side
    own = z - base
    piece = l * cols + x
    is_centre = z == centre
    is_outer = jnp.logical_not(is_centre)
    sibling = y * CORES + (1 - c)
    own_from = min(OWN_FROM, chunks // 2)
    own_fetch = max(0, own_from - 1)
    own_span = max(chunks - own_from - 1, 1)
    share = chunks * width
    lead = min(LEAD, chunks - 1)
    relayed = min(RELAY, chunks - 1)
    begun = min(lead + AHEAD, chunks - 1)
    direct = min(DIRECT, lead + fill + 1)
    ahead = early.shape[1] // (layers * width)
    rounds = d_r.shape[0] - 1
    ready = max(min(PACE, chunks) - 2, min(relayed + group + fill, chunks))
    pace = max(min(PACE, chunks), ready)

    def remote(src, dst, send, recv, **to):
        return pltpu.make_async_remote_copy(
            src_ref=src, dst_ref=dst, send_sem=send, recv_sem=recv, device_id=to, device_id_type=MESH)

    def columns(j, source):
        return pl.ds(pl.multiple_of((source * chunks + j) * width, width), width)

    def early_copy(q):
        src = right.at[:, pl.ds(pl.multiple_of(q * share, width), ahead * width)]
        return pltpu.make_async_copy(src, early.at[:, pl.ds(q * ahead * width, ahead * width)], e_s)

    def local_a():
        return pltpu.make_async_copy(left, a_f32.at[own, piece], a0_s)

    def b_of(j, q):
        if isinstance(j, int) and j < ahead:
            return early.at[:, pl.ds(pl.multiple_of((q * ahead + j) * width, width), width)]
        return right.at[:, columns(j, q)]

    def turn(j):
        return j % b1_r.shape[0] if isinstance(j, int) else lax.rem(j, b1_r.shape[0])

    def b1_local(j):
        return pltpu.make_async_copy(right.at[:, columns(j, l)], b_all.at[j, l, z], b1_r.at[turn(j)])

    for q in range(layers):
        early_copy(q).start()
    local_a().start()
    for j in range(ahead):
        b1_local(j).start()

    barrier = pltpu.get_barrier_semaphore()
    greeted = 0
    for i in range(half):
        row = base + lax.rem(own + i, half)
        for k in range(layers):
            if (i, k) != (0, 0):
                to = {"layer": lax.rem(l + k, layers), "row": row}
                pl.semaphore_signal(barrier, inc=1, device_id=to, device_id_type=MESH)
                greeted += 1
    for k in range(1, cols):
        for m in range(chips):
            to = {"layer": lax.rem(l + m * CORES, layers), "col": lax.rem(x + k, cols)}
            pl.semaphore_signal(barrier, inc=1, device_id=to, device_id_type=MESH)
            greeted += 1

    @pl.when(is_centre)
    def _():
        for i in range(half):
            pl.semaphore_signal(barrier, inc=1, device_id={"row": (1 - side) * half + i}, device_id_type=MESH)
        pl.semaphore_wait(barrier, greeted + half)

    @pl.when(is_outer)
    def _():
        pl.semaphore_signal(barrier, inc=1, device_id={"row": other}, device_id_type=MESH)
        pl.semaphore_wait(barrier, greeted + 1)

    pltpu.make_async_copy(right.at[:, pl.ds(0, layers * ahead * width)], early, e_s).wait()
    local_a().wait()

    def b1(j, k):
        q = lax.rem(l + k, layers)
        return remote(b_of(j, q), b_all.at[j, l, z], b1_s, b1_r.at[turn(j)], layer=q)

    def b1_start(j):
        if not (isinstance(j, int) and j < ahead):
            b1_local(j).start()
        for k in range(1, layers):
            b1(j, k).start()

    def b1_wait(j):
        whole = b_all.at[j, :, z]
        remote(whole, whole, b1_s, b1_r.at[turn(j)], layer=sibling).wait_recv()

    def b1_sent():
        most = right.at[:, pl.ds(0, (layers - 1) * share)]
        remote(most, most, b1_s, b1_r.at[0], layer=sibling).wait_send()

    def slot(j):
        return j % b2_r.shape[0] if isinstance(j, int) else lax.rem(j, b2_r.shape[0])

    def near(j):
        at = b_all.at[j, :, z]
        return remote(at, at, b2_s.at[0], b2_r.at[slot(j), 0], row=centre)

    def far(j):
        at = b_all.at[j, :, z]
        return remote(at, at, b2_s.at[0], b2_r.at[slot(j), 1], row=other)

    def far_part(j, k):
        q = lax.rem(l + k, layers)
        at = b_all.at[j, q, z]
        src = b_of(j, l) if k == 0 else at
        recv = e_r.at[j] if j < fill else b2_r.at[slot(j), 1]
        return remote(src, at, b2_s.at[0], recv, row=other)

    def far_rest(j):
        b1_wait(j)
        if j < direct:
            for k in range(1, layers):
                far_part(j, k).start()
        else:
            far(j).start()

    def fill_send(j, row):
        at = b_all.at[j, :, row]
        remote(at, at, f_s, f_r, row=base + (1 - own)).start()

    def fill_own(j):
        if j < fill:
            fill_send(j, z)

    def fill_far(j):
        if j < fill:
            at = b_all.at[0, :, 0]
            remote(at, at, b2_s.at[0], e_r.at[j], row=other).wait_recv()
            fill_send(j, other)

    def fill_relayed(j):
        if j < fill:
            at = b_all.at[0, :, pl.ds(0, half - 1)]
            remote(at, at, b2_s.at[0], b2_r.at[slot(j), 1], row=other).wait_recv()
            fill_send(j, (1 - side) * (rows - 1))

    def fill_came():
        at = b_all.at[pl.ds(0, fill), :, pl.ds(0, rows - 1)]
        remote(at, at, f_s, f_r, row=centre).wait_recv()

    def fill_sent():
        at = b_all.at[pl.ds(0, fill), :, pl.ds(0, rows - 1)]
        remote(at, at, f_s, f_r, row=centre).wait_send()

    def relay_step(j):
        near = b_all.at[j, :, pl.ds(0, half - 1)]
        remote(near, near, b2_s.at[1], b2_r.at[slot(j), 0], row=other).wait_recv()
        for i in range(1, half):
            at = b_all.at[j, :, base + lax.rem(own + i, half)]
            remote(at, at, b2_s.at[1], b2_r.at[slot(j), 1], row=other).start()

    def b2_wait(j):
        distant = b_all.at[j, :, pl.ds(0, half)]
        remote(distant, distant, b2_s.at[0], b2_r.at[slot(j), 1], row=other).wait_recv()

    def b2_sent():
        at = b_all.at[:, :, 0]
        remote(at, at, b2_s.at[0], b2_r.at[0, 0], row=other).wait_send()

    def relays_sent():
        at = b_all.at[:, :, pl.ds(0, half - 1)]
        remote(at, at, b2_s.at[1], b2_r.at[0, 0], row=other).wait_send()

    def rows_of(t):
        if isinstance(t, int) and t == tiles:
            return pl.ds(0, height)
        return pl.ds(t * fine, fine)

    def a1(t):
        at = a_f32.at[own, piece, rows_of(t)]
        return remote(at, at, a1_s, a1_r.at[(lax.rem(z - centre + half, half) - 1) * tiles + t], row=centre)

    def a1_came(i, t):
        at = a_f32.at[0, 0, rows_of(t)]
        remote(at, at, a1_s, a1_r.at[(i - 1) * tiles + t], row=centre).wait_recv()

    peers = [(m, k) for m in range(chips) for k in range(cols) if (m, k) != (0, 0)]
    everyone = [(0, 0)] + peers

    def a_slot(i, t):
        return 0 if i == 0 else 1 + (i - 1) * tiles + t

    def a2(i, t, m, k):
        to = {"layer": lax.rem(l + m * CORES, layers)}
        if cols > 1:
            to["col"] = lax.rem(x + k, cols)
        at = a_f32.at[lax.rem(own + i, half), piece, rows_of(t)]
        recv = a2_r.at[a_slot(i, t), m * cols + k - 1]
        return remote(at, at, a2_s, recv, **to)

    def a2_came(i, t, m, k):
        at = a_f32.at[0, 0, rows_of(t)]
        remote(at, at, a2_s, a2_r.at[a_slot(i, t), m * cols + k - 1], layer=sibling).wait_recv()

    def a3(i, t, m, k):
        ls = lax.rem(y + chips - m, chips) * CORES + c
        xs = lax.rem(x + cols - k, cols)
        at = a_f32.at[lax.rem(own + i, half), ls * cols + xs, rows_of(t)]
        return remote(at, at, a3_s, a3_r.at[a_slot(i, t)], layer=sibling)

    def a3_came(i, t):
        at = a_f32.at[0, pl.ds(0, chips * cols), rows_of(t)]
        remote(at, at, a3_s, a3_r.at[a_slot(i, t)], layer=sibling).wait_recv()

    def a_sent(count):
        gathered = a_f32.at[pl.ds(0, count), pl.ds(0, len(peers))]
        remote(gathered, gathered, a2_s, a3_r.at[0], layer=sibling).wait_send()
        passed = a_f32.at[pl.ds(0, count), pl.ds(0, len(everyone))]
        remote(passed, passed, a3_s, a3_r.at[0], layer=sibling).wait_send()

    def split_a(s, at):
        for p in range(layers * cols):
            a = a_f32[s, p, at]
            hi = a.astype(jnp.bfloat16)
            a_hi[s, at, p * wide:(p + 1) * wide] = hi
            a_lo[s, at, p * wide:(p + 1) * wide] = (a - hi.astype(jnp.float32)).astype(jnp.bfloat16)

    def split_b(j):
        b = b_all[j].reshape(b_hi.shape)
        hi = b.astype(jnp.bfloat16)
        b_hi[...] = hi
        b_lo[...] = (b - hi.astype(jnp.float32)).astype(jnp.bfloat16)

    def product(j, s, at):
        dot = functools.partial(jnp.dot, preferred_element_type=jnp.float32)
        ah, al = a_hi[s, at, :], a_lo[s, at, :]
        c_buf[j, s, at, :] = dot(al, b_hi[...]) + dot(ah, b_lo[...]) + dot(ah, b_hi[...])

    def block_of(q):
        return pl.ds(pl.multiple_of(q * block, block), block)

    def send_out(j, s, q, mine):
        place = jnp.where(q == l, lax.rem(j // group, rounds), rounds)
        return remote(c_buf.at[j, s, block_of(q)], out.at[:, columns(j, l)],
                      d_s.at[mine], d_r.at[place], layer=q, row=base + s)

    def came_group(g):
        part = out.at[:, pl.ds(0, group * width)]
        remote(part, part, d_s.at[0], d_r.at[lax.rem(g, rounds)], layer=sibling).wait_recv()

    def came_rest():
        part = out.at[:, pl.ds(0, (layers - 1) * share)]
        remote(part, part, d_s.at[0], d_r.at[rounds], layer=sibling).wait_recv()

    def outs_sent():
        theirs = c_buf.at[pl.ds(0, chunks - fill), pl.ds(0, half - 1)]
        remote(theirs, theirs, d_s.at[0], d_r.at[0], layer=sibling).wait_send()
        mine = c_buf.at[:, 0, pl.ds(0, (layers - 1) * block)]
        remote(mine, mine, d_s.at[1], d_r.at[0], layer=sibling).wait_send()

    def product_other(j):
        for i in range(1, half):
            s = lax.rem(own + i, half)

            @pl.loop(0, height // big)
            def _(i):
                t = lax.rem(i + y + c, height // big)
                product(j, s, pl.ds(pl.multiple_of(t * big, big), big))
                for r in range(big // block):
                    send_out(j, s, t * (big // block) + r, 0).start()

    def product_own(j):
        split_b(j)

        @pl.loop(0, height // big)
        def _(t):
            product(j, own, pl.ds(pl.multiple_of(t * big, big), big))
        for k in range(1, layers):
            send_out(j, own, lax.rem(l + k, layers), 1).start()
        out[:, columns(j, l)] = c_buf[j, own, block_of(l), :]

    def fetch_own():
        for m, k in peers:
            a2_came(0, tiles, m, k)
            a3(0, tiles, m, k).start()

    def finish_own():
        a3_came(0, tiles)

        @pl.loop(0, tiles)
        def _(t):
            split_a(own, pl.ds(pl.multiple_of(t * fine, fine), fine))

    def owns(j):
        def upto(n):
            return jnp.maximum(jnp.minimum((n - own_from) * chunks // own_span, n), 0)

        @pl.loop(upto(j), upto(j + 1))
        def _(i):
            product_own(i)

    def own_tile(t):
        for m, k in peers:
            a2(0, t, m, k).start()

    def outer_step(g):
        for i in range(group):
            j = g * group + i

            @pl.when(j + pace < chunks)
            def _():
                b1_start(j + pace)

            @pl.when(j + ready < chunks)
            def _():
                b1_wait(j + ready)
                near(j + ready).start()

    @pl.when(is_outer)
    def _():
        b1_start(0)
        for t in range(min(2, tiles)):
            a1(t).start()
        for j in range(1, pace):
            b1_start(j)
        if fill:
            a3(0, tiles, 0, 0).start()
        for j in range(ready):
            b1_wait(j)
            near(j).start()
            if j == min(1, ready - 1):
                for t in range(2, tiles):
                    a1(t).start()
        first = fill // group

        @pl.loop(first, chunks // group)
        def _(g):
            came_group(g)
            outer_step(g - first)
            if fill:
                n = g - first - 1

                @pl.when(jnp.logical_and(n >= 0, n < tiles))
                def _():
                    own_tile(n)

                @pl.when(n == tiles + 1)
                def _():
                    fetch_own()
                    finish_own()
                    fill_came()

                @pl.when(jnp.logical_and(n > tiles + 1, n <= tiles + 1 + fill))
                def _():
                    product_own(n - tiles - 2)

    @pl.when(is_centre)
    def _():
        b1_start(0)
        for j in range(direct):
            far_part(j, 0).start()
        for j in range(1, min(2, begun + 1)):
            b1_start(j)
        a3(0, tiles, 0, 0).start()
        def spread(t):
            for i in range(1, half):
                a1_came(i, t)
                for m, k in peers:
                    a2(i, t, m, k).start()
                a3(i, t, 0, 0).start()

        def pass_on(t):
            for i in range(1, half):
                for m, k in peers:
                    a2_came(i, t, m, k)
                    a3(i, t, m, k).start()

        spread(0)
        far_rest(0)
        fill_own(0)
        if tiles > 1:
            spread(1)
        for j in range(2, min(3, begun) + 1):
            b1_start(j)
        if lead >= 1:
            far_rest(1)
            fill_own(1)
        relay_step(0)
        fill_far(0)
        pass_on(0)
        if relayed >= 1 and chunks > 2:
            relay_step(1)
        fill_far(1)
        for t in range(2, tiles):
            spread(t)
            if t == 2:
                pass_on(1)
                fill_relayed(0)
        if tiles == 2:
            pass_on(1)
        for j in range(4, begun + 1):
            b1_start(j)
        if lead >= 2:
            far_rest(2)
        fill_relayed(1)
        late = list(range(3, lead + fill + 1))
        relays = list(range(2 if chunks > 2 else 1, relayed + fill + 1))
        if fill > 1:
            for j in relays[:1]:
                relay_step(j)
            for j in late[:1]:
                far_rest(j)
            late, relays = late[1:], relays[1:]

        for t in range(tiles):
            for i in range(1, half):
                if t >= 1 and fill > 1 and t + 1 < tiles:
                    pass_on(t + 1)
                a3_came(i, t)
                split_a(lax.rem(own + i, half), rows_of(t))
            if fill > 1:
                continue
            if t == 0:
                b2_wait(fill)
                split_b(fill)
            for i in range(1, half):
                s = lax.rem(own + i, half)
                product(fill, s, rows_of(t))
                for r in range(fine // block):
                    send_out(fill, s, t * (fine // block) + r, 0).start()
            if t == 0:
                for j in late[:1]:
                    far_rest(j)
                for j in relays[:1]:
                    relay_step(j)
            if 2 <= t + 2 < tiles:
                pass_on(t + 2)
            if t == min(2, tiles - 1):
                for j in late[1:]:
                    far_rest(j)
                for j in relays[1:]:
                    relay_step(j)
        if fill > 1:
            for j in relays[:1]:
                relay_step(j)
            b2_wait(fill)
            split_b(fill)
            product_other(fill)
            for j in late:
                far_rest(j)
            for j in relays[1:]:
                relay_step(j)
        own_tile(0)
        if own_fetch < tiles:
            for t in range(1, tiles):
                own_tile(t)
        if own_from == 0:
            fetch_own()
            finish_own()
            product_own(0)

        @pl.loop(1 + fill, chunks)
        def _(j):
            @pl.when(j + lead + AHEAD - fill < chunks)
            def _():
                b1_start(j + lead + AHEAD - fill)

            @pl.when(j + relayed < chunks)
            def _():
                relay_step(j + relayed)

            @pl.when(j + lead < chunks)
            def _():
                b1_wait(j + lead)
                far(j + lead).start()

            if own_fetch >= tiles:
                @pl.when(j - fill < tiles)
                def _():
                    own_tile(j - fill)

            @pl.when(j == max(own_fetch, 1))
            def _():
                fetch_own()
            b2_wait(j)
            split_b(j)
            product_other(j)

            @pl.when(j == own_from)
            def _():
                finish_own()
            owns(j)

    b1_sent()
    b2_sent()

    @pl.when(is_outer)
    def _():
        remote(left, left, a1_s, a1_r.at[0], row=centre).wait_send()
        if fill:
            a_sent(1)
            mine = c_buf.at[pl.ds(0, fill), 0, pl.ds(0, (layers - 1) * block)]
            remote(mine, mine, d_s.at[1], d_r.at[0], layer=sibling).wait_send()

    @pl.when(is_centre)
    def _():
        a_sent(half)
        if fill:
            fill_sent()
        relays_sent()
        outs_sent()
    came_rest()


def body(mesh, left, right):
    layers, rows, cols = mesh.shape["layer"], mesh.shape["row"], mesh.shape["col"]
    if left.shape[1] % 128:
        left = lax.all_gather(left, "col", axis=1, tiled=True)
        cols = 1
    height, wide = left.shape
    depth, across = right.shape
    share = across // layers
    width = max(128, share // 32)
    chunks = share // width
    half = rows // 2
    inner = depth * layers * rows
    dma = pltpu.SemaphoreType.DMA
    tiles = min(TILES, layers)
    group = GROUP if chunks % GROUP == 0 else 1
    fill = FILL if half == 2 and group == GROUP and chunks // group >= FILL // group + tiles + 3 + FILL else 0
    sizes = (layers, rows, cols, chunks, width, tiles, min(256, height), group, fill)
    chips = layers // CORES
    f32, bf16 = jnp.float32, jnp.bfloat16
    return pl.pallas_call(
        functools.partial(kernel, sizes),
        out_shape=pltpu.VMEM((height // layers, across), f32),
        in_specs=[pl.BlockSpec(memory_space=pltpu.HBM)] * 2,
        out_specs=pl.BlockSpec(memory_space=pltpu.VMEM),
        scratch_shapes=[
            pltpu.VMEM((half, layers * cols, height, wide), f32),
            pltpu.VMEM((half, height, inner), bf16),
            pltpu.VMEM((half, height, inner), bf16),
            pltpu.VMEM((chunks, layers, rows, depth, width), f32),
            pltpu.VMEM((inner, width), bf16),
            pltpu.VMEM((inner, width), bf16),
            pltpu.VMEM((chunks, half, height, width), f32),
            pltpu.VMEM((depth, layers * min(DIRECT, chunks) * width), f32),
            dma, dma, dma, dma(((half - 1) * tiles,)),
            dma, dma(((half - 1) * tiles + 1, chips * cols - 1)), dma, dma(((half - 1) * tiles + 1,)),
            dma, dma((min(16, chunks),)), dma((2,)), dma((min(8, chunks), 2)),
            dma((max(fill, 1),)), dma, dma,
            dma((2,)), dma((min(4, chunks // group) + 1,)),
        ],
        compiler_params=pltpu.CompilerParams(
            collective_id=1, has_side_effects=True, vmem_limit_bytes=53 * 2**20),
    )(left, right)


def solution(mesh):
    in_specs = (P("row", ("layer", "col")), P(("layer", "row"), "col"))
    out_specs = P(("row", "layer"), "col")
    return jax.shard_map(
        functools.partial(body, mesh), mesh=mesh, in_specs=in_specs, out_specs=out_specs, check_vma=False)
```

```python
import functools

import jax
import jax.numpy as jnp
from jax import lax
from jax.experimental import pallas as pl
from jax.experimental.pallas import tpu as pltpu
from jax.sharding import PartitionSpec as P

MESH = pl.DeviceIdType.MESH
CORES = 2
TILES = 4
AHEAD = 4
LEAD = 2
RELAY = 2
OWN_FROM = 7
GROUP = 2
DIRECT = 4
FILL = 2
PACE = 10


def kernel(sizes, left, right, out, a_f32, a_hi, a_lo, b_all, b_hi, b_lo, c_buf, early,
           e_s, a0_s, a1_s, a1_r, a2_s, a2_r, a3_s, a3_r, b1_s, b1_r, b2_s, b2_r, e_r, f_s, f_r, d_s, d_r):
    layers, rows, cols, chunks, width, tiles, big, group, fill = sizes
    half = rows // 2
    chips = layers // CORES
    height, wide = left.shape
    fine = height // tiles
    block = height // layers
    l, z = lax.axis_index("layer"), lax.axis_index("row")
    x = lax.axis_index("col") if cols > 1 else 0
    y, c = l // CORES, l % CORES
    side = z // half
    base = side * half
    centre = half - 1 + side
    other = half - side
    own = z - base
    piece = l * cols + x
    is_centre = z == centre
    is_outer = jnp.logical_not(is_centre)
    sibling = y * CORES + (1 - c)
    own_from = min(OWN_FROM, chunks // 2)
    own_fetch = max(0, own_from - 1)
    own_span = max(chunks - own_from - 1, 1)
    share = chunks * width
    lead = min(LEAD, chunks - 1)
    relayed = min(RELAY, chunks - 1)
    begun = min(lead + AHEAD, chunks - 1)
    direct = min(DIRECT, lead + fill + 1)
    ahead = early.shape[1] // (layers * width)
    rounds = d_r.shape[0] - 1
    ready = max(min(PACE, chunks) - 2, min(relayed + group + fill, chunks))
    pace = max(min(PACE, chunks), ready)

    def remote(src, dst, send, recv, **to):
        return pltpu.make_async_remote_copy(
            src_ref=src, dst_ref=dst, send_sem=send, recv_sem=recv, device_id=to, device_id_type=MESH)

    def columns(j, source):
        return pl.ds(pl.multiple_of((source * chunks + j) * width, width), width)

    def early_copy(q):
        src = right.at[:, pl.ds(pl.multiple_of(q * share, width), ahead * width)]
        return pltpu.make_async_copy(src, early.at[:, pl.ds(q * ahead * width, ahead * width)], e_s)

    def local_a():
        return pltpu.make_async_copy(left, a_f32.at[own, piece], a0_s)

    def b_of(j, q):
        if isinstance(j, int) and j < ahead:
            return early.at[:, pl.ds(pl.multiple_of((q * ahead + j) * width, width), width)]
        return right.at[:, columns(j, q)]

    def turn(j):
        return j % b1_r.shape[0] if isinstance(j, int) else lax.rem(j, b1_r.shape[0])

    def b1_local(j):
        return pltpu.make_async_copy(right.at[:, columns(j, l)], b_all.at[j, l, z], b1_r.at[turn(j)])

    for q in range(layers):
        early_copy(q).start()
    local_a().start()
    for j in range(ahead):
        b1_local(j).start()

    barrier = pltpu.get_barrier_semaphore()
    greeted = 0
    for i in range(half):
        row = base + lax.rem(own + i, half)
        for k in range(layers):
            if (i, k) != (0, 0):
                to = {"layer": lax.rem(l + k, layers), "row": row}
                pl.semaphore_signal(barrier, inc=1, device_id=to, device_id_type=MESH)
                greeted += 1
    for k in range(1, cols):
        for m in range(chips):
            to = {"layer": lax.rem(l + m * CORES, layers), "col": lax.rem(x + k, cols)}
            pl.semaphore_signal(barrier, inc=1, device_id=to, device_id_type=MESH)
            greeted += 1

    @pl.when(is_centre)
    def _():
        for i in range(half):
            pl.semaphore_signal(barrier, inc=1, device_id={"row": (1 - side) * half + i}, device_id_type=MESH)
        pl.semaphore_wait(barrier, greeted + half)

    @pl.when(is_outer)
    def _():
        pl.semaphore_signal(barrier, inc=1, device_id={"row": other}, device_id_type=MESH)
        pl.semaphore_wait(barrier, greeted + 1)

    pltpu.make_async_copy(right.at[:, pl.ds(0, layers * ahead * width)], early, e_s).wait()
    local_a().wait()

    def b1(j, k):
        q = lax.rem(l + k, layers)
        return remote(b_of(j, q), b_all.at[j, l, z], b1_s, b1_r.at[turn(j)], layer=q)

    def b1_start(j):
        if not (isinstance(j, int) and j < ahead):
            b1_local(j).start()
        for k in range(1, layers):
            b1(j, k).start()

    def b1_wait(j):
        whole = b_all.at[j, :, z]
        remote(whole, whole, b1_s, b1_r.at[turn(j)], layer=sibling).wait_recv()

    def b1_sent():
        most = right.at[:, pl.ds(0, (layers - 1) * share)]
        remote(most, most, b1_s, b1_r.at[0], layer=sibling).wait_send()

    def slot(j):
        return j % b2_r.shape[0] if isinstance(j, int) else lax.rem(j, b2_r.shape[0])

    def near(j):
        at = b_all.at[j, :, z]
        return remote(at, at, b2_s.at[0], b2_r.at[slot(j), 0], row=centre)

    def far(j):
        at = b_all.at[j, :, z]
        return remote(at, at, b2_s.at[0], b2_r.at[slot(j), 1], row=other)

    def far_part(j, k):
        q = lax.rem(l + k, layers)
        at = b_all.at[j, q, z]
        src = b_of(j, l) if k == 0 else at
        recv = e_r.at[j] if j < fill else b2_r.at[slot(j), 1]
        return remote(src, at, b2_s.at[0], recv, row=other)

    def far_rest(j):
        b1_wait(j)
        if j < direct:
            for k in range(1, layers):
                far_part(j, k).start()
        else:
            far(j).start()

    def fill_send(j, row):
        at = b_all.at[j, :, row]
        remote(at, at, f_s, f_r, row=base + (1 - own)).start()

    def fill_own(j):
        if j < fill:
            fill_send(j, z)

    def fill_far(j):
        if j < fill:
            at = b_all.at[0, :, 0]
            remote(at, at, b2_s.at[0], e_r.at[j], row=other).wait_recv()
            fill_send(j, other)

    def fill_relayed(j):
        if j < fill:
            at = b_all.at[0, :, pl.ds(0, half - 1)]
            remote(at, at, b2_s.at[0], b2_r.at[slot(j), 1], row=other).wait_recv()
            fill_send(j, (1 - side) * (rows - 1))

    def fill_came():
        at = b_all.at[pl.ds(0, fill), :, pl.ds(0, rows - 1)]
        remote(at, at, f_s, f_r, row=centre).wait_recv()

    def fill_sent():
        at = b_all.at[pl.ds(0, fill), :, pl.ds(0, rows - 1)]
        remote(at, at, f_s, f_r, row=centre).wait_send()

    def relay_step(j):
        near = b_all.at[j, :, pl.ds(0, half - 1)]
        remote(near, near, b2_s.at[1], b2_r.at[slot(j), 0], row=other).wait_recv()
        for i in range(1, half):
            at = b_all.at[j, :, base + lax.rem(own + i, half)]
            remote(at, at, b2_s.at[1], b2_r.at[slot(j), 1], row=other).start()

    def b2_wait(j):
        distant = b_all.at[j, :, pl.ds(0, half)]
        remote(distant, distant, b2_s.at[0], b2_r.at[slot(j), 1], row=other).wait_recv()

    def b2_sent():
        at = b_all.at[:, :, 0]
        remote(at, at, b2_s.at[0], b2_r.at[0, 0], row=other).wait_send()

    def relays_sent():
        at = b_all.at[:, :, pl.ds(0, half - 1)]
        remote(at, at, b2_s.at[1], b2_r.at[0, 0], row=other).wait_send()

    def rows_of(t):
        if isinstance(t, int) and t == tiles:
            return pl.ds(0, height)
        return pl.ds(t * fine, fine)

    def a1(t):
        at = a_f32.at[own, piece, rows_of(t)]
        return remote(at, at, a1_s, a1_r.at[(lax.rem(z - centre + half, half) - 1) * tiles + t], row=centre)

    def a1_came(i, t):
        at = a_f32.at[0, 0, rows_of(t)]
        remote(at, at, a1_s, a1_r.at[(i - 1) * tiles + t], row=centre).wait_recv()

    peers = [(m, k) for m in range(chips) for k in range(cols) if (m, k) != (0, 0)]
    everyone = [(0, 0)] + peers

    def a_slot(i, t):
        return 0 if i == 0 else 1 + (i - 1) * tiles + t

    def a2(i, t, m, k):
        to = {"layer": lax.rem(l + m * CORES, layers)}
        if cols > 1:
            to["col"] = lax.rem(x + k, cols)
        at = a_f32.at[lax.rem(own + i, half), piece, rows_of(t)]
        recv = a2_r.at[a_slot(i, t), m * cols + k - 1]
        return remote(at, at, a2_s, recv, **to)

    def a2_came(i, t, m, k):
        at = a_f32.at[0, 0, rows_of(t)]
        remote(at, at, a2_s, a2_r.at[a_slot(i, t), m * cols + k - 1], layer=sibling).wait_recv()

    def a3(i, t, m, k):
        ls = lax.rem(y + chips - m, chips) * CORES + c
        xs = lax.rem(x + cols - k, cols)
        at = a_f32.at[lax.rem(own + i, half), ls * cols + xs, rows_of(t)]
        return remote(at, at, a3_s, a3_r.at[a_slot(i, t)], layer=sibling)

    def a3_came(i, t):
        at = a_f32.at[0, pl.ds(0, chips * cols), rows_of(t)]
        remote(at, at, a3_s, a3_r.at[a_slot(i, t)], layer=sibling).wait_recv()

    def a_sent(count):
        gathered = a_f32.at[pl.ds(0, count), pl.ds(0, len(peers))]
        remote(gathered, gathered, a2_s, a3_r.at[0], layer=sibling).wait_send()
        passed = a_f32.at[pl.ds(0, count), pl.ds(0, len(everyone))]
        remote(passed, passed, a3_s, a3_r.at[0], layer=sibling).wait_send()

    def split_a(s, at):
        for p in range(layers * cols):
            a = a_f32[s, p, at]
            hi = a.astype(jnp.bfloat16)
            a_hi[s, at, p * wide:(p + 1) * wide] = hi
            a_lo[s, at, p * wide:(p + 1) * wide] = (a - hi.astype(jnp.float32)).astype(jnp.bfloat16)

    def split_b(j):
        b = b_all[j].reshape(b_hi.shape)
        hi = b.astype(jnp.bfloat16)
        b_hi[...] = hi
        b_lo[...] = (b - hi.astype(jnp.float32)).astype(jnp.bfloat16)

    def product(j, s, at):
        dot = functools.partial(jnp.dot, preferred_element_type=jnp.float32)
        ah, al = a_hi[s, at, :], a_lo[s, at, :]
        c_buf[j, s, at, :] = dot(al, b_hi[...]) + dot(ah, b_lo[...]) + dot(ah, b_hi[...])

    def block_of(q):
        return pl.ds(pl.multiple_of(q * block, block), block)

    def send_out(j, s, q, mine):
        place = jnp.where(q == l, lax.rem(j // group, rounds), rounds)
        return remote(c_buf.at[j, s, block_of(q)], out.at[:, columns(j, l)],
                      d_s.at[mine], d_r.at[place], layer=q, row=base + s)

    def came_group(g):
        part = out.at[:, pl.ds(0, group * width)]
        remote(part, part, d_s.at[0], d_r.at[lax.rem(g, rounds)], layer=sibling).wait_recv()

    def came_rest():
        part = out.at[:, pl.ds(0, (layers - 1) * share)]
        remote(part, part, d_s.at[0], d_r.at[rounds], layer=sibling).wait_recv()

    def outs_sent():
        theirs = c_buf.at[pl.ds(0, chunks - fill), pl.ds(0, half - 1)]
        remote(theirs, theirs, d_s.at[0], d_r.at[0], layer=sibling).wait_send()
        mine = c_buf.at[:, 0, pl.ds(0, (layers - 1) * block)]
        remote(mine, mine, d_s.at[1], d_r.at[0], layer=sibling).wait_send()

    def product_other(j):
        for i in range(1, half):
            s = lax.rem(own + i, half)

            @pl.loop(0, height // big)
            def _(i):
                t = lax.rem(i + y + c, height // big)
                product(j, s, pl.ds(pl.multiple_of(t * big, big), big))
                for r in range(big // block):
                    send_out(j, s, t * (big // block) + r, 0).start()

    def product_own(j):
        split_b(j)

        @pl.loop(0, height // big)
        def _(t):
            product(j, own, pl.ds(pl.multiple_of(t * big, big), big))
        for k in range(1, layers):
            send_out(j, own, lax.rem(l + k, layers), 1).start()
        out[:, columns(j, l)] = c_buf[j, own, block_of(l), :]

    def fetch_own():
        for m, k in peers:
            a2_came(0, tiles, m, k)
            a3(0, tiles, m, k).start()

    def finish_own():
        a3_came(0, tiles)

        @pl.loop(0, tiles)
        def _(t):
            split_a(own, pl.ds(pl.multiple_of(t * fine, fine), fine))

    def owns(j):
        def upto(n):
            return jnp.maximum(jnp.minimum((n - own_from) * chunks // own_span, n), 0)

        @pl.loop(upto(j), upto(j + 1))
        def _(i):
            product_own(i)

    def own_tile(t):
        for m, k in peers:
            a2(0, t, m, k).start()

    def outer_step(g):
        for i in range(group):
            j = g * group + i

            @pl.when(j + pace < chunks)
            def _():
                b1_start(j + pace)

            @pl.when(j + ready < chunks)
            def _():
                b1_wait(j + ready)
                near(j + ready).start()

    @pl.when(is_outer)
    def _():
        b1_start(0)
        for t in range(min(2, tiles)):
            a1(t).start()
        for j in range(1, pace):
            b1_start(j)
        if fill:
            a3(0, tiles, 0, 0).start()
        for j in range(ready):
            b1_wait(j)
            near(j).start()
            if j >= 1 and 1 + j < tiles:
                a1(1 + j).start()
        for t in range(max(ready + 1, 2), tiles):
            a1(t).start()
        first = fill // group

        @pl.loop(first, chunks // group)
        def _(g):
            came_group(g)
            outer_step(g - first)
            if fill:
                n = g - first - 1

                @pl.when(jnp.logical_and(n >= 0, n < tiles))
                def _():
                    own_tile(n)

                @pl.when(n == tiles + 1)
                def _():
                    fetch_own()
                    finish_own()
                    fill_came()

                @pl.when(jnp.logical_and(n > tiles + 1, n <= tiles + 1 + fill))
                def _():
                    product_own(n - tiles - 2)

    @pl.when(is_centre)
    def _():
        b1_start(0)
        for j in range(direct):
            far_part(j, 0).start()
        for j in range(1, min(2, begun + 1)):
            b1_start(j)
        a3(0, tiles, 0, 0).start()
        def spread(t):
            for i in range(1, half):
                a1_came(i, t)
                for m, k in peers:
                    a2(i, t, m, k).start()
                a3(i, t, 0, 0).start()

        def pass_on(t):
            for i in range(1, half):
                for m, k in peers:
                    a2_came(i, t, m, k)
                    a3(i, t, m, k).start()

        spread(0)
        far_rest(0)
        fill_own(0)
        if tiles > 1:
            spread(1)
        for j in range(2, min(3, begun) + 1):
            b1_start(j)
        if lead >= 1:
            far_rest(1)
            fill_own(1)
        relay_step(0)
        fill_far(0)
        pass_on(0)
        if relayed >= 1 and chunks > 2:
            relay_step(1)
        fill_far(1)
        if tiles > 2:
            spread(2)
        if tiles > 1:
            pass_on(1)
        fill_relayed(0)
        if lead >= 2:
            far_rest(2)
        if fill > 1:
            relay_step(2)
        for t in range(3, tiles):
            spread(t)
        fill_relayed(1)
        late = list(range(3, lead + fill + 1))
        relays = list(range(max(fill + 1, 2) if chunks > 2 else 1, relayed + fill + 1))
        for j in late[:1]:
            far_rest(j)
        for j in range(4, begun + 1):
            b1_start(j)

        per = max(1, big // fine)
        for t in range(tiles):
            for i in range(1, half):
                if t >= 3:
                    pass_on(t)
                a3_came(i, t)
                split_a(lax.rem(own + i, half), rows_of(t))
            if t == min(1, per - 1) and tiles > 2:
                pass_on(2)
            if t == per - 1:
                for j in relays[:1]:
                    relay_step(j)
                b2_wait(fill)
                split_b(fill)
            if t % per == per - 1:
                for i in range(1, half):
                    s = lax.rem(own + i, half)
                    product(fill, s, pl.ds((t + 1 - per) * fine, per * fine))
                    for q in range((t + 1 - per) * fine // block, (t + 1) * fine // block):
                        send_out(fill, s, q, 0).start()
        for j in late[1:]:
            far_rest(j)
        for j in relays[1:]:
            relay_step(j)
        own_tile(0)
        if own_fetch < tiles:
            for t in range(1, tiles):
                own_tile(t)
        if own_from == 0:
            fetch_own()
            finish_own()
            product_own(0)

        @pl.loop(1 + fill, chunks)
        def _(j):
            @pl.when(j + lead + AHEAD - fill < chunks)
            def _():
                b1_start(j + lead + AHEAD - fill)

            @pl.when(j + relayed < chunks)
            def _():
                relay_step(j + relayed)

            @pl.when(j + lead < chunks)
            def _():
                b1_wait(j + lead)
                far(j + lead).start()

            if own_fetch >= tiles:
                @pl.when(j - fill < tiles)
                def _():
                    own_tile(j - fill)

            @pl.when(j == max(own_fetch, 1))
            def _():
                fetch_own()
            b2_wait(j)
            split_b(j)
            product_other(j)

            @pl.when(j == own_from)
            def _():
                finish_own()
            owns(j)

    b1_sent()
    b2_sent()

    @pl.when(is_outer)
    def _():
        remote(left, left, a1_s, a1_r.at[0], row=centre).wait_send()
        if fill:
            a_sent(1)
            mine = c_buf.at[pl.ds(0, fill), 0, pl.ds(0, (layers - 1) * block)]
            remote(mine, mine, d_s.at[1], d_r.at[0], layer=sibling).wait_send()

    @pl.when(is_centre)
    def _():
        a_sent(half)
        if fill:
            fill_sent()
        relays_sent()
        outs_sent()
    came_rest()


def body(mesh, left, right):
    layers, rows, cols = mesh.shape["layer"], mesh.shape["row"], mesh.shape["col"]
    if left.shape[1] % 128:
        left = lax.all_gather(left, "col", axis=1, tiled=True)
        cols = 1
    height, wide = left.shape
    depth, across = right.shape
    share = across // layers
    width = max(128, share // 32)
    chunks = share // width
    half = rows // 2
    inner = depth * layers * rows
    dma = pltpu.SemaphoreType.DMA
    tiles = min(TILES, layers)
    group = GROUP if chunks % GROUP == 0 else 1
    fill = FILL if half == 2 and group == GROUP and chunks // group >= FILL // group + tiles + 3 + FILL else 0
    sizes = (layers, rows, cols, chunks, width, tiles, min(256, height), group, fill)
    chips = layers // CORES
    f32, bf16 = jnp.float32, jnp.bfloat16
    return pl.pallas_call(
        functools.partial(kernel, sizes),
        out_shape=pltpu.VMEM((height // layers, across), f32),
        in_specs=[pl.BlockSpec(memory_space=pltpu.HBM)] * 2,
        out_specs=pl.BlockSpec(memory_space=pltpu.VMEM),
        scratch_shapes=[
            pltpu.VMEM((half, layers * cols, height, wide), f32),
            pltpu.VMEM((half, height, inner), bf16),
            pltpu.VMEM((half, height, inner), bf16),
            pltpu.VMEM((chunks, layers, rows, depth, width), f32),
            pltpu.VMEM((inner, width), bf16),
            pltpu.VMEM((inner, width), bf16),
            pltpu.VMEM((chunks, half, height, width), f32),
            pltpu.VMEM((depth, layers * min(DIRECT, chunks) * width), f32),
            dma, dma, dma, dma(((half - 1) * tiles,)),
            dma, dma(((half - 1) * tiles + 1, chips * cols - 1)), dma, dma(((half - 1) * tiles + 1,)),
            dma, dma((min(16, chunks),)), dma((2,)), dma((min(8, chunks), 2)),
            dma((max(fill, 1),)), dma, dma,
            dma((2,)), dma((min(4, chunks // group) + 1,)),
        ],
        compiler_params=pltpu.CompilerParams(
            collective_id=1, has_side_effects=True, vmem_limit_bytes=53 * 2**20),
    )(left, right)


def solution(mesh):
    in_specs = (P("row", ("layer", "col")), P(("layer", "row"), "col"))
    out_specs = P(("row", "layer"), "col")
    return jax.shard_map(
        functools.partial(body, mesh), mesh=mesh, in_specs=in_specs, out_specs=out_specs, check_vma=False)
```

```python
import functools

import jax
import jax.numpy as jnp
from jax import lax
from jax.experimental import pallas as pl
from jax.experimental.pallas import tpu as pltpu
from jax.sharding import PartitionSpec as P

MESH = pl.DeviceIdType.MESH
CORES = 2
TILES = 4
AHEAD = 4
LEAD = 2
RELAY = 2
OWN_FROM = 7
GROUP = 2
DIRECT = 4
FILL = 2
HASTY = 2
PACE = 10


def kernel(sizes, left, right, out, a_f32, a_hi, a_lo, b_all, b_hi, b_lo, c_buf, early,
           e_s, a0_s, a1_s, a1_r, a2_s, a2_r, a3_s, a3_r, b1_s, b1_r, b2_s, b2_r, e_r, f_s, f_r, d_s, d_r):
    layers, rows, cols, chunks, width, tiles, big, group, fill = sizes
    half = rows // 2
    chips = layers // CORES
    height, wide = left.shape
    fine = height // tiles
    block = height // layers
    l, z = lax.axis_index("layer"), lax.axis_index("row")
    x = lax.axis_index("col") if cols > 1 else 0
    y, c = l // CORES, l % CORES
    side = z // half
    base = side * half
    centre = half - 1 + side
    other = half - side
    own = z - base
    piece = l * cols + x
    is_centre = z == centre
    is_outer = jnp.logical_not(is_centre)
    sibling = y * CORES + (1 - c)
    own_from = min(OWN_FROM, chunks // 2)
    own_fetch = max(0, own_from - 1)
    own_span = max(chunks - own_from - 1, 1)
    share = chunks * width
    lead = min(LEAD, chunks - 1)
    relayed = min(RELAY, chunks - 1)
    begun = min(lead + AHEAD, chunks - 1)
    direct = min(DIRECT, lead + fill + 1)
    ahead = early.shape[1] // (layers * width)
    rounds = d_r.shape[0] - 1
    hasty = min(HASTY, ahead)
    ready = max(min(PACE, chunks) - 2, min(relayed + group + fill, chunks))
    pace = max(min(PACE, chunks), ready)

    def remote(src, dst, send, recv, **to):
        return pltpu.make_async_remote_copy(
            src_ref=src, dst_ref=dst, send_sem=send, recv_sem=recv, device_id=to, device_id_type=MESH)

    def columns(j, source):
        return pl.ds(pl.multiple_of((source * chunks + j) * width, width), width)

    def early_copy(q):
        src = right.at[:, pl.ds(pl.multiple_of(q * share, width), ahead * width)]
        return pltpu.make_async_copy(src, early.at[:, pl.ds(q * ahead * width, ahead * width)], e_s)

    def local_a():
        return pltpu.make_async_copy(left, a_f32.at[own, piece], a0_s)

    def b_of(j, q):
        if isinstance(j, int) and j < ahead:
            return early.at[:, pl.ds(pl.multiple_of((q * ahead + j) * width, width), width)]
        return right.at[:, columns(j, q)]

    def turn(j):
        return j % b1_r.shape[0] if isinstance(j, int) else lax.rem(j, b1_r.shape[0])

    def b1_local(j):
        return pltpu.make_async_copy(right.at[:, columns(j, l)], b_all.at[j, l, z], b1_r.at[turn(j)])

    for q in range(layers):
        early_copy(q).start()
    local_a().start()
    for j in range(ahead):
        b1_local(j).start()

    barrier = pltpu.get_barrier_semaphore()
    greeted = 0
    for i in range(half):
        row = base + lax.rem(own + i, half)
        for k in range(layers):
            if (i, k) != (0, 0):
                to = {"layer": lax.rem(l + k, layers), "row": row}
                pl.semaphore_signal(barrier, inc=1, device_id=to, device_id_type=MESH)
                greeted += 1
    for k in range(1, cols):
        for m in range(chips):
            to = {"layer": lax.rem(l + m * CORES, layers), "col": lax.rem(x + k, cols)}
            pl.semaphore_signal(barrier, inc=1, device_id=to, device_id_type=MESH)
            greeted += 1

    @pl.when(is_centre)
    def _():
        for i in range(half):
            pl.semaphore_signal(barrier, inc=1, device_id={"row": (1 - side) * half + i}, device_id_type=MESH)
        pl.semaphore_wait(barrier, greeted + half)

    @pl.when(is_outer)
    def _():
        pl.semaphore_signal(barrier, inc=1, device_id={"row": other}, device_id_type=MESH)
        pl.semaphore_wait(barrier, greeted + 1)

    pltpu.make_async_copy(right.at[:, pl.ds(0, layers * ahead * width)], early, e_s).wait()
    local_a().wait()

    def b1(j, k):
        q = lax.rem(l + k, layers)
        return remote(b_of(j, q), b_all.at[j, l, z], b1_s, b1_r.at[turn(j)], layer=q)

    def b1_start(j):
        if not (isinstance(j, int) and j < ahead):
            b1_local(j).start()
        for k in range(1, layers):
            b1(j, k).start()

    def b1_wait(j):
        whole = b_all.at[j, :, z]
        remote(whole, whole, b1_s, b1_r.at[turn(j)], layer=sibling).wait_recv()

    def b1_sent():
        most = right.at[:, pl.ds(0, (layers - 1) * share)]
        remote(most, most, b1_s, b1_r.at[0], layer=sibling).wait_send()

    def slot(j):
        return j % b2_r.shape[0] if isinstance(j, int) else lax.rem(j, b2_r.shape[0])

    def near(j):
        at = b_all.at[j, :, z]
        return remote(at, at, b2_s.at[0], b2_r.at[slot(j), 0], row=centre)

    def near_part(j, k):
        q = lax.rem(l + k, layers)
        at = b_all.at[j, q, z]
        src = b_of(j, l) if k == 0 else at
        return remote(src, at, b2_s.at[0], b2_r.at[slot(j), 0], row=centre)

    def near_rest(j):
        b1_wait(j)
        if j < hasty:
            for k in range(1, layers):
                near_part(j, k).start()
        else:
            near(j).start()

    def far(j):
        at = b_all.at[j, :, z]
        return remote(at, at, b2_s.at[0], b2_r.at[slot(j), 1], row=other)

    def far_part(j, k):
        q = lax.rem(l + k, layers)
        at = b_all.at[j, q, z]
        src = b_of(j, l) if k == 0 else at
        recv = e_r.at[j] if j < fill else b2_r.at[slot(j), 1]
        return remote(src, at, b2_s.at[0], recv, row=other)

    def far_rest(j):
        b1_wait(j)
        if j < direct:
            for k in range(1, layers):
                far_part(j, k).start()
        else:
            far(j).start()

    def fill_send(j, row):
        at = b_all.at[j, :, row]
        remote(at, at, f_s, f_r, row=base + (1 - own)).start()

    def fill_own(j):
        if j < fill:
            fill_send(j, z)

    def fill_far(j):
        if j < fill:
            at = b_all.at[0, :, 0]
            remote(at, at, b2_s.at[0], e_r.at[j], row=other).wait_recv()
            fill_send(j, other)

    def fill_relayed(j):
        if j < fill:
            at = b_all.at[0, :, pl.ds(0, half - 1)]
            remote(at, at, b2_s.at[0], b2_r.at[slot(j), 1], row=other).wait_recv()
            fill_send(j, (1 - side) * (rows - 1))

    def fill_came():
        at = b_all.at[pl.ds(0, fill), :, pl.ds(0, rows - 1)]
        remote(at, at, f_s, f_r, row=centre).wait_recv()

    def fill_sent():
        at = b_all.at[pl.ds(0, fill), :, pl.ds(0, rows - 1)]
        remote(at, at, f_s, f_r, row=centre).wait_send()

    def relay_step(j):
        near = b_all.at[j, :, pl.ds(0, half - 1)]
        remote(near, near, b2_s.at[1], b2_r.at[slot(j), 0], row=other).wait_recv()
        for i in range(1, half):
            at = b_all.at[j, :, base + lax.rem(own + i, half)]
            remote(at, at, b2_s.at[1], b2_r.at[slot(j), 1], row=other).start()

    def b2_wait(j):
        distant = b_all.at[j, :, pl.ds(0, half)]
        remote(distant, distant, b2_s.at[0], b2_r.at[slot(j), 1], row=other).wait_recv()

    def b2_sent():
        at = b_all.at[:, :, 0]
        remote(at, at, b2_s.at[0], b2_r.at[0, 0], row=other).wait_send()

    def relays_sent():
        at = b_all.at[:, :, pl.ds(0, half - 1)]
        remote(at, at, b2_s.at[1], b2_r.at[0, 0], row=other).wait_send()

    def rows_of(t):
        if isinstance(t, int) and t == tiles:
            return pl.ds(0, height)
        return pl.ds(t * fine, fine)

    def a1(t):
        at = a_f32.at[own, piece, rows_of(t)]
        return remote(at, at, a1_s, a1_r.at[(lax.rem(z - centre + half, half) - 1) * tiles + t], row=centre)

    def a1_came(i, t):
        at = a_f32.at[0, 0, rows_of(t)]
        remote(at, at, a1_s, a1_r.at[(i - 1) * tiles + t], row=centre).wait_recv()

    peers = [(m, k) for m in range(chips) for k in range(cols) if (m, k) != (0, 0)]
    everyone = [(0, 0)] + peers

    def a_slot(i, t):
        return 0 if i == 0 else 1 + (i - 1) * tiles + t

    def a2(i, t, m, k):
        to = {"layer": lax.rem(l + m * CORES, layers)}
        if cols > 1:
            to["col"] = lax.rem(x + k, cols)
        at = a_f32.at[lax.rem(own + i, half), piece, rows_of(t)]
        recv = a2_r.at[a_slot(i, t), m * cols + k - 1]
        return remote(at, at, a2_s, recv, **to)

    def a2_came(i, t, m, k):
        at = a_f32.at[0, 0, rows_of(t)]
        remote(at, at, a2_s, a2_r.at[a_slot(i, t), m * cols + k - 1], layer=sibling).wait_recv()

    def a3(i, t, m, k):
        ls = lax.rem(y + chips - m, chips) * CORES + c
        xs = lax.rem(x + cols - k, cols)
        at = a_f32.at[lax.rem(own + i, half), ls * cols + xs, rows_of(t)]
        return remote(at, at, a3_s, a3_r.at[a_slot(i, t)], layer=sibling)

    def a3_came(i, t):
        at = a_f32.at[0, pl.ds(0, chips * cols), rows_of(t)]
        remote(at, at, a3_s, a3_r.at[a_slot(i, t)], layer=sibling).wait_recv()

    def a_sent(count):
        gathered = a_f32.at[pl.ds(0, count), pl.ds(0, len(peers))]
        remote(gathered, gathered, a2_s, a3_r.at[0], layer=sibling).wait_send()
        passed = a_f32.at[pl.ds(0, count), pl.ds(0, len(everyone))]
        remote(passed, passed, a3_s, a3_r.at[0], layer=sibling).wait_send()

    def split_a(s, at):
        for p in range(layers * cols):
            a = a_f32[s, p, at]
            hi = a.astype(jnp.bfloat16)
            a_hi[s, at, p * wide:(p + 1) * wide] = hi
            a_lo[s, at, p * wide:(p + 1) * wide] = (a - hi.astype(jnp.float32)).astype(jnp.bfloat16)

    def split_b(j):
        b = b_all[j].reshape(b_hi.shape)
        hi = b.astype(jnp.bfloat16)
        b_hi[...] = hi
        b_lo[...] = (b - hi.astype(jnp.float32)).astype(jnp.bfloat16)

    def product(j, s, at):
        dot = functools.partial(jnp.dot, preferred_element_type=jnp.float32)
        ah, al = a_hi[s, at, :], a_lo[s, at, :]
        c_buf[j, s, at, :] = dot(al, b_hi[...]) + dot(ah, b_lo[...]) + dot(ah, b_hi[...])

    def block_of(q):
        return pl.ds(pl.multiple_of(q * block, block), block)

    def send_out(j, s, q, mine):
        place = jnp.where(q == l, lax.rem(j // group, rounds), rounds)
        return remote(c_buf.at[j, s, block_of(q)], out.at[:, columns(j, l)],
                      d_s.at[mine], d_r.at[place], layer=q, row=base + s)

    def came_group(g):
        part = out.at[:, pl.ds(0, group * width)]
        remote(part, part, d_s.at[0], d_r.at[lax.rem(g, rounds)], layer=sibling).wait_recv()

    def came_rest():
        part = out.at[:, pl.ds(0, (layers - 1) * share)]
        remote(part, part, d_s.at[0], d_r.at[rounds], layer=sibling).wait_recv()

    def outs_sent():
        theirs = c_buf.at[pl.ds(0, chunks - fill), pl.ds(0, half - 1)]
        remote(theirs, theirs, d_s.at[0], d_r.at[0], layer=sibling).wait_send()
        mine = c_buf.at[:, 0, pl.ds(0, (layers - 1) * block)]
        remote(mine, mine, d_s.at[1], d_r.at[0], layer=sibling).wait_send()

    def product_other(j):
        for i in range(1, half):
            s = lax.rem(own + i, half)

            @pl.loop(0, height // big)
            def _(i):
                t = lax.rem(i + y + c, height // big)
                product(j, s, pl.ds(pl.multiple_of(t * big, big), big))
                for r in range(big // block):
                    send_out(j, s, t * (big // block) + r, 0).start()

    def product_own(j):
        split_b(j)

        @pl.loop(0, height // big)
        def _(t):
            product(j, own, pl.ds(pl.multiple_of(t * big, big), big))
        for k in range(1, layers):
            send_out(j, own, lax.rem(l + k, layers), 1).start()
        out[:, columns(j, l)] = c_buf[j, own, block_of(l), :]

    def fetch_own():
        for m, k in peers:
            a2_came(0, tiles, m, k)
            a3(0, tiles, m, k).start()

    def finish_own():
        a3_came(0, tiles)

        @pl.loop(0, tiles)
        def _(t):
            split_a(own, pl.ds(pl.multiple_of(t * fine, fine), fine))

    def owns(j):
        def upto(n):
            return jnp.maximum(jnp.minimum((n - own_from) * chunks // own_span, n), 0)

        @pl.loop(upto(j), upto(j + 1))
        def _(i):
            product_own(i)

    def own_tile(t):
        for m, k in peers:
            a2(0, t, m, k).start()

    def outer_step(g):
        for i in range(group):
            j = g * group + i

            @pl.when(j + pace < chunks)
            def _():
                b1_start(j + pace)

            @pl.when(j + ready < chunks)
            def _():
                b1_wait(j + ready)
                near(j + ready).start()

    @pl.when(is_outer)
    def _():
        b1_start(0)
        for t in range(min(2, tiles)):
            a1(t).start()
        for j in range(hasty):
            near_part(j, 0).start()
        for j in range(1, pace):
            b1_start(j)
        if fill:
            a3(0, tiles, 0, 0).start()
        for j in range(ready):
            near_rest(j)
            if j >= 1 and 1 + j < tiles:
                a1(1 + j).start()
        for t in range(max(ready + 1, 2), tiles):
            a1(t).start()
        first = fill // group

        @pl.loop(first, chunks // group)
        def _(g):
            came_group(g)
            outer_step(g - first)
            if fill:
                n = g - first - 1

                @pl.when(jnp.logical_and(n >= 0, n < tiles))
                def _():
                    own_tile(n)

                @pl.when(n == tiles + 1)
                def _():
                    fetch_own()
                    finish_own()
                    fill_came()

                @pl.when(jnp.logical_and(n > tiles + 1, n <= tiles + 1 + fill))
                def _():
                    product_own(n - tiles - 2)

    @pl.when(is_centre)
    def _():
        b1_start(0)
        for j in range(direct):
            far_part(j, 0).start()
        for j in range(1, min(2, begun + 1)):
            b1_start(j)
        a3(0, tiles, 0, 0).start()
        def spread(t):
            for i in range(1, half):
                a1_came(i, t)
                for m, k in peers:
                    a2(i, t, m, k).start()
                a3(i, t, 0, 0).start()

        def pass_on(t):
            for i in range(1, half):
                for m, k in peers:
                    a2_came(i, t, m, k)
                    a3(i, t, m, k).start()

        spread(0)
        far_rest(0)
        fill_own(0)
        if tiles > 1:
            spread(1)
        for j in range(2, min(3, begun) + 1):
            b1_start(j)
        if lead >= 1:
            far_rest(1)
            fill_own(1)
        relay_step(0)
        fill_far(0)
        pass_on(0)
        if relayed >= 1 and chunks > 2:
            relay_step(1)
        fill_far(1)
        if tiles > 2:
            spread(2)
        if tiles > 1:
            pass_on(1)
        fill_relayed(0)
        if lead >= 2:
            far_rest(2)
        if fill > 1:
            relay_step(2)
        for t in range(3, tiles):
            spread(t)
        fill_relayed(1)
        late = list(range(3, lead + fill + 1))
        relays = list(range(max(fill + 1, 2) if chunks > 2 else 1, relayed + fill + 1))
        for j in late[:1]:
            far_rest(j)
        for j in range(4, begun + 1):
            b1_start(j)

        per = max(1, big // fine)
        for t in range(tiles):
            for i in range(1, half):
                if t >= 3:
                    pass_on(t)
                a3_came(i, t)
                split_a(lax.rem(own + i, half), rows_of(t))
            if t == min(1, per - 1) and tiles > 2:
                pass_on(2)
            if t == per - 1:
                for j in relays[:1]:
                    relay_step(j)
                b2_wait(fill)
                split_b(fill)
            if t % per == per - 1:
                for i in range(1, half):
                    s = lax.rem(own + i, half)
                    product(fill, s, pl.ds((t + 1 - per) * fine, per * fine))
                    for q in range((t + 1 - per) * fine // block, (t + 1) * fine // block):
                        send_out(fill, s, q, 0).start()
        for j in late[1:]:
            far_rest(j)
        for j in relays[1:]:
            relay_step(j)
        own_tile(0)
        if own_fetch < tiles:
            for t in range(1, tiles):
                own_tile(t)
        if own_from == 0:
            fetch_own()
            finish_own()
            product_own(0)

        @pl.loop(1 + fill, chunks)
        def _(j):
            @pl.when(j + lead + AHEAD - fill < chunks)
            def _():
                b1_start(j + lead + AHEAD - fill)

            @pl.when(j + relayed < chunks)
            def _():
                relay_step(j + relayed)

            @pl.when(j + lead < chunks)
            def _():
                b1_wait(j + lead)
                far(j + lead).start()

            if own_fetch >= tiles:
                @pl.when(j - fill < tiles)
                def _():
                    own_tile(j - fill)

            @pl.when(j == max(own_fetch, 1))
            def _():
                fetch_own()
            b2_wait(j)
            split_b(j)
            product_other(j)

            @pl.when(j == own_from)
            def _():
                finish_own()
            owns(j)

    b1_sent()
    b2_sent()

    @pl.when(is_outer)
    def _():
        remote(left, left, a1_s, a1_r.at[0], row=centre).wait_send()
        if fill:
            a_sent(1)
            mine = c_buf.at[pl.ds(0, fill), 0, pl.ds(0, (layers - 1) * block)]
            remote(mine, mine, d_s.at[1], d_r.at[0], layer=sibling).wait_send()

    @pl.when(is_centre)
    def _():
        a_sent(half)
        if fill:
            fill_sent()
        relays_sent()
        outs_sent()
    came_rest()


def body(mesh, left, right):
    layers, rows, cols = mesh.shape["layer"], mesh.shape["row"], mesh.shape["col"]
    if left.shape[1] % 128:
        left = lax.all_gather(left, "col", axis=1, tiled=True)
        cols = 1
    height, wide = left.shape
    depth, across = right.shape
    share = across // layers
    width = max(128, share // 32)
    chunks = share // width
    half = rows // 2
    inner = depth * layers * rows
    dma = pltpu.SemaphoreType.DMA
    tiles = min(TILES, layers)
    group = GROUP if chunks % GROUP == 0 else 1
    fill = FILL if half == 2 and group == GROUP and chunks // group >= FILL // group + tiles + 3 + FILL else 0
    sizes = (layers, rows, cols, chunks, width, tiles, min(256, height), group, fill)
    chips = layers // CORES
    f32, bf16 = jnp.float32, jnp.bfloat16
    return pl.pallas_call(
        functools.partial(kernel, sizes),
        out_shape=pltpu.VMEM((height // layers, across), f32),
        in_specs=[pl.BlockSpec(memory_space=pltpu.HBM)] * 2,
        out_specs=pl.BlockSpec(memory_space=pltpu.VMEM),
        scratch_shapes=[
            pltpu.VMEM((half, layers * cols, height, wide), f32),
            pltpu.VMEM((half, height, inner), bf16),
            pltpu.VMEM((half, height, inner), bf16),
            pltpu.VMEM((chunks, layers, rows, depth, width), f32),
            pltpu.VMEM((inner, width), bf16),
            pltpu.VMEM((inner, width), bf16),
            pltpu.VMEM((chunks, half, height, width), f32),
            pltpu.VMEM((depth, layers * min(DIRECT, chunks) * width), f32),
            dma, dma, dma, dma(((half - 1) * tiles,)),
            dma, dma(((half - 1) * tiles + 1, chips * cols - 1)), dma, dma(((half - 1) * tiles + 1,)),
            dma, dma((min(16, chunks),)), dma((2,)), dma((min(8, chunks), 2)),
            dma((max(fill, 1),)), dma, dma,
            dma((2,)), dma((min(4, chunks // group) + 1,)),
        ],
        compiler_params=pltpu.CompilerParams(
            collective_id=1, has_side_effects=True, vmem_limit_bytes=53 * 2**20),
    )(left, right)


def solution(mesh):
    in_specs = (P("row", ("layer", "col")), P(("layer", "row"), "col"))
    out_specs = P(("row", "layer"), "col")
    return jax.shard_map(
        functools.partial(body, mesh), mesh=mesh, in_specs=in_specs, out_specs=out_specs, check_vma=False)
```

```python
import functools

import jax
import jax.numpy as jnp
from jax import lax
from jax.experimental import pallas as pl
from jax.experimental.pallas import tpu as pltpu
from jax.sharding import PartitionSpec as P

MESH = pl.DeviceIdType.MESH
CORES = 2
TILES = 4
AHEAD = 4
LEAD = 2
RELAY = 2
OWN_FROM = 7
GROUP = 2
DIRECT = 4
FILL = 2
HASTY = 2
PACE = 10


def kernel(sizes, left, right, out, a_f32, a_hi, a_lo, b_all, b_hi, b_lo, c_buf, early,
           e_s, a0_s, a1_s, a1_r, a2_s, a2_r, a3_s, a3_r, b1_s, b1_r, b2_s, b2_r, e_r, f_s, f_r, d_s, d_r):
    layers, rows, cols, chunks, width, tiles, big, group, fill = sizes
    half = rows // 2
    chips = layers // CORES
    height, wide = left.shape
    fine = height // tiles
    block = height // layers
    l, z = lax.axis_index("layer"), lax.axis_index("row")
    x = lax.axis_index("col") if cols > 1 else 0
    y, c = l // CORES, l % CORES
    side = z // half
    base = side * half
    centre = half - 1 + side
    other = half - side
    own = z - base
    piece = l * cols + x
    is_centre = z == centre
    is_outer = jnp.logical_not(is_centre)
    sibling = y * CORES + (1 - c)
    own_from = min(OWN_FROM, chunks // 2)
    own_fetch = max(0, own_from - 1)
    own_span = max(chunks - own_from - 1, 1)
    share = chunks * width
    lead = min(LEAD, chunks - 1)
    relayed = min(RELAY, chunks - 1)
    begun = min(lead + AHEAD, chunks - 1)
    direct = min(DIRECT, lead + fill + 1)
    ahead = early.shape[1] // (layers * width)
    rounds = d_r.shape[0] - 1
    hasty = min(HASTY, ahead)
    ready = max(min(PACE, chunks) - 2, min(relayed + group + fill, chunks))
    pace = max(min(PACE, chunks), ready)

    def remote(src, dst, send, recv, **to):
        return pltpu.make_async_remote_copy(
            src_ref=src, dst_ref=dst, send_sem=send, recv_sem=recv, device_id=to, device_id_type=MESH)

    def columns(j, source):
        return pl.ds(pl.multiple_of((source * chunks + j) * width, width), width)

    def early_copy(q):
        src = right.at[:, pl.ds(pl.multiple_of(q * share, width), ahead * width)]
        return pltpu.make_async_copy(src, early.at[:, pl.ds(q * ahead * width, ahead * width)], e_s)

    def local_a():
        return pltpu.make_async_copy(left, a_f32.at[own, piece], a0_s)

    def b_of(j, q):
        if isinstance(j, int) and j < ahead:
            return early.at[:, pl.ds(pl.multiple_of((q * ahead + j) * width, width), width)]
        return right.at[:, columns(j, q)]

    def turn(j):
        return j % b1_r.shape[0] if isinstance(j, int) else lax.rem(j, b1_r.shape[0])

    def b1_local(j):
        return pltpu.make_async_copy(right.at[:, columns(j, l)], b_all.at[j, l, z], b1_r.at[turn(j)])

    for q in range(layers):
        early_copy(q).start()
    local_a().start()
    for j in range(ahead):
        b1_local(j).start()

    barrier = pltpu.get_barrier_semaphore()
    greeted = 0
    for k in range(1, layers):
        pl.semaphore_signal(barrier, inc=1, device_id={"layer": lax.rem(l + k, layers)}, device_id_type=MESH)
        greeted += 1
    for k in range(1, half):
        row = base + lax.rem(own + k, half)
        pl.semaphore_signal(barrier, inc=1, device_id={"row": row}, device_id_type=MESH)
        greeted += 1
    for k in range(1, cols):
        pl.semaphore_signal(barrier, inc=1, device_id={"col": lax.rem(x + k, cols)}, device_id_type=MESH)
        greeted += 1

    @pl.when(is_centre)
    def _():
        pl.semaphore_signal(barrier, inc=1, device_id={"row": other}, device_id_type=MESH)
        pl.semaphore_wait(barrier, greeted + 1)

    @pl.when(is_outer)
    def _():
        pl.semaphore_wait(barrier, greeted)

    pltpu.make_async_copy(right.at[:, pl.ds(0, layers * ahead * width)], early, e_s).wait()
    local_a().wait()

    def b1(j, k):
        q = lax.rem(l + k, layers)
        return remote(b_of(j, q), b_all.at[j, l, z], b1_s, b1_r.at[turn(j)], layer=q)

    def b1_start(j):
        if not (isinstance(j, int) and j < ahead):
            b1_local(j).start()
        for k in range(1, layers):
            b1(j, k).start()

    def b1_wait(j):
        whole = b_all.at[j, :, z]
        remote(whole, whole, b1_s, b1_r.at[turn(j)], layer=sibling).wait_recv()

    def b1_sent():
        most = right.at[:, pl.ds(0, (layers - 1) * share)]
        remote(most, most, b1_s, b1_r.at[0], layer=sibling).wait_send()

    def slot(j):
        return j % b2_r.shape[0] if isinstance(j, int) else lax.rem(j, b2_r.shape[0])

    def near(j):
        at = b_all.at[j, :, z]
        return remote(at, at, b2_s.at[0], b2_r.at[slot(j), 0], row=centre)

    def near_part(j, k):
        q = lax.rem(l + k, layers)
        at = b_all.at[j, q, z]
        src = b_of(j, l) if k == 0 else at
        return remote(src, at, b2_s.at[0], b2_r.at[slot(j), 0], row=centre)

    def near_rest(j):
        b1_wait(j)
        if j < hasty:
            for k in range(1, layers):
                near_part(j, k).start()
        else:
            near(j).start()

    def far(j):
        at = b_all.at[j, :, z]
        return remote(at, at, b2_s.at[0], b2_r.at[slot(j), 1], row=other)

    def far_part(j, k):
        q = lax.rem(l + k, layers)
        at = b_all.at[j, q, z]
        src = b_of(j, l) if k == 0 else at
        recv = e_r.at[j] if j < fill else b2_r.at[slot(j), 1]
        return remote(src, at, b2_s.at[0], recv, row=other)

    def far_rest(j):
        b1_wait(j)
        if j < direct:
            for k in range(1, layers):
                far_part(j, k).start()
        else:
            far(j).start()

    def fill_send(j, row):
        at = b_all.at[j, :, row]
        remote(at, at, f_s, f_r, row=base + (1 - own)).start()

    def fill_own(j):
        if j < fill:
            fill_send(j, z)

    def fill_far(j):
        if j < fill:
            at = b_all.at[0, :, 0]
            remote(at, at, b2_s.at[0], e_r.at[j], row=other).wait_recv()
            fill_send(j, other)

    def fill_relayed(j):
        if j < fill:
            at = b_all.at[0, :, pl.ds(0, half - 1)]
            remote(at, at, b2_s.at[0], b2_r.at[slot(j), 1], row=other).wait_recv()
            fill_send(j, (1 - side) * (rows - 1))

    def fill_came():
        at = b_all.at[pl.ds(0, fill), :, pl.ds(0, rows - 1)]
        remote(at, at, f_s, f_r, row=centre).wait_recv()

    def fill_sent():
        at = b_all.at[pl.ds(0, fill), :, pl.ds(0, rows - 1)]
        remote(at, at, f_s, f_r, row=centre).wait_send()

    def relay_step(j):
        near = b_all.at[j, :, pl.ds(0, half - 1)]
        remote(near, near, b2_s.at[1], b2_r.at[slot(j), 0], row=other).wait_recv()
        for i in range(1, half):
            at = b_all.at[j, :, base + lax.rem(own + i, half)]
            remote(at, at, b2_s.at[1], b2_r.at[slot(j), 1], row=other).start()

    def b2_wait(j):
        distant = b_all.at[j, :, pl.ds(0, half)]
        remote(distant, distant, b2_s.at[0], b2_r.at[slot(j), 1], row=other).wait_recv()

    def b2_sent():
        at = b_all.at[:, :, 0]
        remote(at, at, b2_s.at[0], b2_r.at[0, 0], row=other).wait_send()

    def relays_sent():
        at = b_all.at[:, :, pl.ds(0, half - 1)]
        remote(at, at, b2_s.at[1], b2_r.at[0, 0], row=other).wait_send()

    def rows_of(t):
        if isinstance(t, int) and t == tiles:
            return pl.ds(0, height)
        return pl.ds(t * fine, fine)

    def a1(t):
        at = a_f32.at[own, piece, rows_of(t)]
        return remote(at, at, a1_s, a1_r.at[(lax.rem(z - centre + half, half) - 1) * tiles + t], row=centre)

    def a1_came(i, t):
        at = a_f32.at[0, 0, rows_of(t)]
        remote(at, at, a1_s, a1_r.at[(i - 1) * tiles + t], row=centre).wait_recv()

    peers = [(m, k) for m in range(chips) for k in range(cols) if (m, k) != (0, 0)]
    everyone = [(0, 0)] + peers

    def a_slot(i, t):
        return 0 if i == 0 else 1 + (i - 1) * tiles + t

    def a2(i, t, m, k):
        to = {"layer": lax.rem(l + m * CORES, layers)}
        if cols > 1:
            to["col"] = lax.rem(x + k, cols)
        at = a_f32.at[lax.rem(own + i, half), piece, rows_of(t)]
        recv = a2_r.at[a_slot(i, t), m * cols + k - 1]
        return remote(at, at, a2_s, recv, **to)

    def a2_came(i, t, m, k):
        at = a_f32.at[0, 0, rows_of(t)]
        remote(at, at, a2_s, a2_r.at[a_slot(i, t), m * cols + k - 1], layer=sibling).wait_recv()

    def a3(i, t, m, k):
        ls = lax.rem(y + chips - m, chips) * CORES + c
        xs = lax.rem(x + cols - k, cols)
        at = a_f32.at[lax.rem(own + i, half), ls * cols + xs, rows_of(t)]
        return remote(at, at, a3_s, a3_r.at[a_slot(i, t)], layer=sibling)

    def a3_came(i, t):
        at = a_f32.at[0, pl.ds(0, chips * cols), rows_of(t)]
        remote(at, at, a3_s, a3_r.at[a_slot(i, t)], layer=sibling).wait_recv()

    def a_sent(count):
        gathered = a_f32.at[pl.ds(0, count), pl.ds(0, len(peers))]
        remote(gathered, gathered, a2_s, a3_r.at[0], layer=sibling).wait_send()
        passed = a_f32.at[pl.ds(0, count), pl.ds(0, len(everyone))]
        remote(passed, passed, a3_s, a3_r.at[0], layer=sibling).wait_send()

    def split_a(s, at):
        for p in range(layers * cols):
            a = a_f32[s, p, at]
            hi = a.astype(jnp.bfloat16)
            a_hi[s, at, p * wide:(p + 1) * wide] = hi
            a_lo[s, at, p * wide:(p + 1) * wide] = (a - hi.astype(jnp.float32)).astype(jnp.bfloat16)

    def split_b(j):
        b = b_all[j].reshape(b_hi.shape)
        hi = b.astype(jnp.bfloat16)
        b_hi[...] = hi
        b_lo[...] = (b - hi.astype(jnp.float32)).astype(jnp.bfloat16)

    def product(j, s, at):
        dot = functools.partial(jnp.dot, preferred_element_type=jnp.float32)
        ah, al = a_hi[s, at, :], a_lo[s, at, :]
        c_buf[j, s, at, :] = dot(al, b_hi[...]) + dot(ah, b_lo[...]) + dot(ah, b_hi[...])

    def block_of(q):
        return pl.ds(pl.multiple_of(q * block, block), block)

    def send_out(j, s, q, mine):
        place = jnp.where(q == l, lax.rem(j // group, rounds), rounds)
        return remote(c_buf.at[j, s, block_of(q)], out.at[:, columns(j, l)],
                      d_s.at[mine], d_r.at[place], layer=q, row=base + s)

    def came_group(g):
        part = out.at[:, pl.ds(0, group * width)]
        remote(part, part, d_s.at[0], d_r.at[lax.rem(g, rounds)], layer=sibling).wait_recv()

    def came_rest():
        part = out.at[:, pl.ds(0, (layers - 1) * share)]
        remote(part, part, d_s.at[0], d_r.at[rounds], layer=sibling).wait_recv()

    def outs_sent():
        theirs = c_buf.at[pl.ds(0, chunks - fill), pl.ds(0, half - 1)]
        remote(theirs, theirs, d_s.at[0], d_r.at[0], layer=sibling).wait_send()
        mine = c_buf.at[:, 0, pl.ds(0, (layers - 1) * block)]
        remote(mine, mine, d_s.at[1], d_r.at[0], layer=sibling).wait_send()

    def product_other(j):
        for i in range(1, half):
            s = lax.rem(own + i, half)

            @pl.loop(0, height // big)
            def _(i):
                t = lax.rem(i + y + c, height // big)
                product(j, s, pl.ds(pl.multiple_of(t * big, big), big))
                for r in range(big // block):
                    send_out(j, s, t * (big // block) + r, 0).start()

    def product_own(j):
        split_b(j)

        @pl.loop(0, height // big)
        def _(t):
            product(j, own, pl.ds(pl.multiple_of(t * big, big), big))
        for k in range(1, layers):
            send_out(j, own, lax.rem(l + k, layers), 1).start()
        out[:, columns(j, l)] = c_buf[j, own, block_of(l), :]

    def fetch_own():
        for m, k in peers:
            a2_came(0, tiles, m, k)
            a3(0, tiles, m, k).start()

    def finish_own():
        a3_came(0, tiles)

        @pl.loop(0, tiles)
        def _(t):
            split_a(own, pl.ds(pl.multiple_of(t * fine, fine), fine))

    def owns(j):
        def upto(n):
            return jnp.maximum(jnp.minimum((n - own_from) * chunks // own_span, n), 0)

        @pl.loop(upto(j), upto(j + 1))
        def _(i):
            product_own(i)

    def own_tile(t):
        for m, k in peers:
            a2(0, t, m, k).start()

    def outer_step(g):
        for i in range(group):
            j = g * group + i

            @pl.when(j + pace < chunks)
            def _():
                b1_start(j + pace)

            @pl.when(j + ready < chunks)
            def _():
                b1_wait(j + ready)
                near(j + ready).start()

    @pl.when(is_outer)
    def _():
        b1_start(0)
        for t in range(min(2, tiles)):
            a1(t).start()
        for j in range(hasty):
            near_part(j, 0).start()
        for j in range(1, pace):
            b1_start(j)
        if fill:
            a3(0, tiles, 0, 0).start()
        for j in range(ready):
            near_rest(j)
            if j >= 1 and 1 + j < tiles:
                a1(1 + j).start()
        for t in range(max(ready + 1, 2), tiles):
            a1(t).start()
        first = fill // group

        @pl.loop(first, chunks // group)
        def _(g):
            came_group(g)
            outer_step(g - first)
            if fill:
                n = g - first - 1

                @pl.when(jnp.logical_and(n >= 0, n < tiles))
                def _():
                    own_tile(n)

                @pl.when(n == tiles + 1)
                def _():
                    fetch_own()
                    finish_own()
                    fill_came()

                @pl.when(jnp.logical_and(n > tiles + 1, n <= tiles + 1 + fill))
                def _():
                    product_own(n - tiles - 2)

    @pl.when(is_centre)
    def _():
        b1_start(0)
        for j in range(direct):
            far_part(j, 0).start()
        for j in range(1, min(2, begun + 1)):
            b1_start(j)
        a3(0, tiles, 0, 0).start()
        def spread(t):
            for i in range(1, half):
                a1_came(i, t)
                for m, k in peers:
                    a2(i, t, m, k).start()
                a3(i, t, 0, 0).start()

        def pass_on(t):
            for i in range(1, half):
                for m, k in peers:
                    a2_came(i, t, m, k)
                    a3(i, t, m, k).start()

        far_rest(0)
        spread(0)
        fill_own(0)
        if tiles > 1:
            spread(1)
        for j in range(2, min(3, begun) + 1):
            b1_start(j)
        if lead >= 1:
            far_rest(1)
            fill_own(1)
        relay_step(0)
        fill_far(0)
        pass_on(0)
        if relayed >= 1 and chunks > 2:
            relay_step(1)
        fill_far(1)
        if tiles > 2:
            spread(2)
        if tiles > 1:
            pass_on(1)
        fill_relayed(0)
        if lead >= 2:
            far_rest(2)
        if fill > 1:
            relay_step(2)
        for t in range(3, tiles):
            spread(t)
        fill_relayed(1)
        late = list(range(3, lead + fill + 1))
        relays = list(range(max(fill + 1, 2) if chunks > 2 else 1, relayed + fill + 1))
        for j in late[:1]:
            far_rest(j)
        for j in range(4, begun + 1):
            b1_start(j)

        per = max(1, big // fine)
        for t in range(tiles):
            for i in range(1, half):
                if t >= 3:
                    pass_on(t)
                a3_came(i, t)
                split_a(lax.rem(own + i, half), rows_of(t))
            if t == min(1, per - 1) and tiles > 2:
                pass_on(2)
            if t == per - 1:
                for j in relays[:1]:
                    relay_step(j)
                b2_wait(fill)
                split_b(fill)
            if t % per == per - 1:
                for i in range(1, half):
                    s = lax.rem(own + i, half)
                    product(fill, s, pl.ds((t + 1 - per) * fine, per * fine))
                    for q in range((t + 1 - per) * fine // block, (t + 1) * fine // block):
                        send_out(fill, s, q, 0).start()
        for j in late[1:]:
            far_rest(j)
        for j in relays[1:]:
            relay_step(j)
        own_tile(0)
        if own_fetch < tiles:
            for t in range(1, tiles):
                own_tile(t)
        if own_from == 0:
            fetch_own()
            finish_own()
            product_own(0)

        @pl.loop(1 + fill, chunks)
        def _(j):
            @pl.when(j + lead + AHEAD - fill < chunks)
            def _():
                b1_start(j + lead + AHEAD - fill)

            @pl.when(j + relayed < chunks)
            def _():
                relay_step(j + relayed)

            @pl.when(j + lead < chunks)
            def _():
                b1_wait(j + lead)
                far(j + lead).start()

            if own_fetch >= tiles:
                @pl.when(j - fill < tiles)
                def _():
                    own_tile(j - fill)

            @pl.when(j == max(own_fetch, 1))
            def _():
                fetch_own()
            b2_wait(j)
            split_b(j)
            product_other(j)

            @pl.when(j == own_from)
            def _():
                finish_own()
            owns(j)

    b1_sent()
    b2_sent()

    @pl.when(is_outer)
    def _():
        remote(left, left, a1_s, a1_r.at[0], row=centre).wait_send()
        if fill:
            a_sent(1)
            mine = c_buf.at[pl.ds(0, fill), 0, pl.ds(0, (layers - 1) * block)]
            remote(mine, mine, d_s.at[1], d_r.at[0], layer=sibling).wait_send()

    @pl.when(is_centre)
    def _():
        a_sent(half)
        if fill:
            fill_sent()
        relays_sent()
        outs_sent()
    came_rest()


def body(mesh, left, right):
    layers, rows, cols = mesh.shape["layer"], mesh.shape["row"], mesh.shape["col"]
    if left.shape[1] % 128:
        left = lax.all_gather(left, "col", axis=1, tiled=True)
        cols = 1
    height, wide = left.shape
    depth, across = right.shape
    share = across // layers
    width = max(128, share // 32)
    chunks = share // width
    half = rows // 2
    inner = depth * layers * rows
    dma = pltpu.SemaphoreType.DMA
    tiles = min(TILES, layers)
    group = GROUP if chunks % GROUP == 0 else 1
    fill = FILL if half == 2 and group == GROUP and chunks // group >= FILL // group + tiles + 3 + FILL else 0
    sizes = (layers, rows, cols, chunks, width, tiles, min(256, height), group, fill)
    chips = layers // CORES
    f32, bf16 = jnp.float32, jnp.bfloat16
    return pl.pallas_call(
        functools.partial(kernel, sizes),
        out_shape=pltpu.VMEM((height // layers, across), f32),
        in_specs=[pl.BlockSpec(memory_space=pltpu.HBM)] * 2,
        out_specs=pl.BlockSpec(memory_space=pltpu.VMEM),
        scratch_shapes=[
            pltpu.VMEM((half, layers * cols, height, wide), f32),
            pltpu.VMEM((half, height, inner), bf16),
            pltpu.VMEM((half, height, inner), bf16),
            pltpu.VMEM((chunks, layers, rows, depth, width), f32),
            pltpu.VMEM((inner, width), bf16),
            pltpu.VMEM((inner, width), bf16),
            pltpu.VMEM((chunks, half, height, width), f32),
            pltpu.VMEM((depth, layers * min(DIRECT, chunks) * width), f32),
            dma, dma, dma, dma(((half - 1) * tiles,)),
            dma, dma(((half - 1) * tiles + 1, chips * cols - 1)), dma, dma(((half - 1) * tiles + 1,)),
            dma, dma((min(16, chunks),)), dma((2,)), dma((min(8, chunks), 2)),
            dma((max(fill, 1),)), dma, dma,
            dma((2,)), dma((min(4, chunks // group) + 1,)),
        ],
        compiler_params=pltpu.CompilerParams(
            collective_id=1, has_side_effects=True, vmem_limit_bytes=53 * 2**20),
    )(left, right)


def solution(mesh):
    in_specs = (P("row", ("layer", "col")), P(("layer", "row"), "col"))
    out_specs = P(("row", "layer"), "col")
    return jax.shard_map(
        functools.partial(body, mesh), mesh=mesh, in_specs=in_specs, out_specs=out_specs, check_vma=False)
```
